512 devices in a mesh: dp: 64 (over x, z), head: 8 (over y, core).
Axes of the slice: x: 4, y: 4, z: 16, core: 2. Of those that a mesh axis runs over, the one named last changes fastest.
Arguments:
- gradients: float32 [3, 32, 64, 65536], P(None, 'head', None, 'dp'), may hold values from -0.6777015 to 0.6777015
- preconditioner: float32 [3, 32, 64, 64], P(None, 'head'), may hold values from -0.75 to 0.75
- partners: int32 [256, 7], P('dp'), may hold values from -1 to 255, as said below
Outputs:
- tiles: float32 [256, 256, 7, 256], P('head', 'dp')
The draws below stay inside these ranges and needn't reach their ends.
Inputs may be any that keep to these rules, and one draw needn't show every extreme that they name: `partners`: blocks fall into clusters of consecutive blocks, each of at most 8 blocks; row a lists the blocks after a in its cluster in ascending order (slot k holds a + k + 1), then -1 in the remaining slots, so every unordered pair of distinct blocks of a cluster appears once. Some block has all 7 slots filled.
All inputs are finite; a program needn't handle non-finite values.
Results may differ from the reference program's by a relative error of at most 0.013.
Values may be sent and summed in bfloat16 or wider, within the bound.
A program may use at most 64 MiB of HBM per device.

```python
import jax
import jax.numpy as jnp
from jax import lax

HEADS = 32
HEAD_DIM = 64
LAYERS = 3
BS = 256
BLOCKS_DEV = 4
REACH = 7
N_BLOCKS = 256
EXAMPLES = 65536
N_HEAD = 8


def draw_partners(key, part):
    key_offset, key_extra, key_chosen = jax.random.split(jax.random.fold_in(key, 17), 3)
    cluster_most = REACH + 1
    grid_offset = jax.random.randint(key_offset, (), 1, BLOCKS_DEV)
    position = jnp.arange(N_BLOCKS, dtype=jnp.int32)
    on_grid = (position - grid_offset) % cluster_most == 0
    extra_start = jax.random.randint(key_extra, (N_BLOCKS,), 0, 24) == 0
    choices_left = (N_BLOCKS - grid_offset) // cluster_most
    chosen = grid_offset + cluster_most * jax.random.randint(key_chosen, (), 0, choices_left)
    inside = (position > chosen) & (position < chosen + cluster_most)
    starts = (on_grid | extra_start | (position == 0) | (position == chosen)) & jnp.logical_not(inside)
    cluster = jnp.cumsum(starts.astype(jnp.int32))
    step_ahead = jnp.arange(1, REACH + 1, dtype=jnp.int32)
    target = position[:, None] + step_ahead[None, :]
    clipped = jnp.minimum(target, N_BLOCKS - 1)
    same_cluster = (target < N_BLOCKS) & (cluster[clipped] == cluster[:, None])
    return jnp.where(same_cluster, target, -1).astype(jnp.int32)


def steps_of(own_key, shape, cuts, low, high):
    gain = 1.0
    for dim, blocks in cuts:
        steps = jax.random.uniform(jax.random.fold_in(jax.random.fold_in(own_key, 6), dim), (blocks,), jnp.float32, low / len(cuts), high / len(cuts))
        gain = gain * jnp.repeat(jnp.exp(steps), shape[dim] // blocks).reshape((-1,) + (1,) * (len(shape) - 1 - dim))
    return gain


def centred(rng, dims, scale, most, cuts=(), held_as=jnp.bfloat16):
    loudness = steps_of(rng, dims, cuts, -0.22, 0.18) if cuts else 1.0
    entries = jax.random.normal(rng, dims, jnp.float32) * scale * loudness
    return jnp.minimum(jnp.maximum(entries, -most), most).astype(held_as)


def setup_inputs(seed: int = 0) -> dict:
    streams_of = jax.random.split(jax.random.key(seed), 4)
    return {
        "gradients": centred(streams_of[0], (LAYERS, HEADS, HEAD_DIM, EXAMPLES), ((LAYERS * HEADS * HEAD_DIM) ** -0.25), 0.6777015, ((1, 8), (3, 64)), jnp.float32),
        "preconditioner": centred(streams_of[1], (LAYERS, HEADS, HEAD_DIM, HEAD_DIM), HEAD_DIM ** -0.5, 0.75, ((1, 8),), jnp.float32),
        "partners": draw_partners(jax.random.fold_in(streams_of[3], 71), 0),
    }


def reference(gradients, preconditioner, partners):
    layers, head_count, head_depth, examples = gradients.shape
    blocks = examples // BS
    group_heads = head_count // N_HEAD
    group_rows = layers * group_heads * head_depth
    scaled = jnp.einsum("lhde,lhdn->lhen", preconditioner, gradients, precision=lax.Precision.HIGHEST)

    def grouped(values):
        rounded = values.astype(jnp.bfloat16)
        shaped = rounded.reshape(layers, N_HEAD, group_heads, head_depth, blocks, BS)
        return shaped.transpose(1, 0, 2, 3, 4, 5).reshape(N_HEAD, group_rows, blocks, BS)

    scaled_groups = grouped(scaled)
    plain_groups = grouped(gradients)

    def one_block(block_index):
        own_rows = jnp.take(scaled_groups, block_index, axis=2).astype(jnp.float32)
        partner_ids = partners[block_index]
        clamped = jnp.maximum(partner_ids, 0).astype(jnp.int32)
        partner_cols = jnp.take(plain_groups, clamped, axis=2).astype(jnp.float32)
        partial_value = jnp.einsum("gci,gckj->gikj", own_rows, partner_cols, precision=lax.Precision.HIGHEST)
        live_slot = (partner_ids >= 0).astype(jnp.float32)
        partial_value = (partial_value * live_slot[None, None, :, None]).astype(jnp.bfloat16).astype(jnp.float32)
        return jnp.sum(partial_value, axis=0)

    tiles = lax.map(one_block, jnp.arange(blocks, dtype=jnp.int32))
    return tiles.transpose(1, 0, 2, 3)
```

```python
import functools

import jax
import jax.numpy as jnp
from jax import lax
from jax.experimental import pallas as pl
from jax.experimental.pallas import tpu as pltpu
from jax.sharding import PartitionSpec as P

MESH = pl.DeviceIdType.MESH
BF16 = jnp.bfloat16
F32 = jnp.float32

BS = 256
NB = 4
SLOTS = 7
ROWS = 768
LAYERS = 3
LROWS = ROWS // LAYERS
HD = 64
NY = 4
HALF = BS // 2
PIECE = HALF // NY

STAGES = (
    (tuple(("own", a, b) for b in range(1, NB) for a in range(b)), BS),
    (tuple(("own", a, 4) for a in range(NB)), BS),
    (
        tuple(("own", a, 5) for a in range(NB))
        + (("far", 3, 0), ("far", 2, 0), ("far", 3, 1), ("far", 2, 1)),
        BS,
    ),
    (tuple(("own", a, 6) for a in range(NB)) + (("far", 1, 0), ("far", 3, 2)), BS),
    (tuple(("own", a, 7) for a in range(NB)), BS // 2),
    (tuple(("own", a, 7) for a in range(NB)), BS // 2),
)
COLUMN0 = (0, 0, 0, 0, 0, BS // 2)
NSTAGE = len(STAGES)


def kernel(g_hbm, p_ref, out_ref, *scratch):
    (gbuf, plain, scaled, from_next, from_next_half, from_prev, ship0, ship1, far0, far1) = scratch[:10]
    stage_refs = [scratch[10 + 5 * s : 15 + 5 * s] for s in range(NSTAGE)]
    (
        load_sem,
        left_send,
        left_recv,
        right_send,
        right_recv,
        core_send,
        core_recv,
        y_send,
        y_recv,
        far_send,
        far_recv,
    ) = scratch[10 + 5 * NSTAGE :]
    ships, fars = {2: ship0, 3: ship1}, {2: far0, 3: far1}

    n_dp = lax.axis_size("dp")
    dp = lax.axis_index("dp")
    head = lax.axis_index("head")
    core = lax.rem(head, 2)
    y = lax.div(head, 2)
    previous = lax.rem(dp + n_dp - 1, n_dp)
    following = lax.rem(dp + 1, n_dp)
    other = head + 1 - 2 * core
    peers = [lax.rem(y + d, NY) * 2 + core for d in range(1, NY)]

    loads = []
    for j in range(NB):
        load = pltpu.make_async_copy(g_hbm.at[:, pl.ds(j * BS, BS)], gbuf.at[j], load_sem.at[j])
        load.start()
        loads.append(load)

    barrier = pltpu.get_barrier_semaphore()
    for target in (previous, following):
        pl.semaphore_signal(barrier, inc=1, device_id={"dp": target}, device_id_type=MESH)
    for target in [other] + peers:
        pl.semaphore_signal(barrier, inc=1, device_id={"head": target}, device_id_type=MESH)

    pending = []

    def send(src, dst, send_sem, recv_sem, device):
        copy = pltpu.make_async_remote_copy(
            src_ref=src,
            dst_ref=dst,
            send_sem=send_sem,
            recv_sem=recv_sem,
            device_id=device,
            device_id_type=MESH,
        )
        copy.start()
        pending.append(copy)
        return copy

    left = []
    for j in range(NB):
        loads[j].wait()
        plain[j] = gbuf[j].astype(BF16)
        if j == 0:
            pl.semaphore_wait(barrier, 2 + 1 + len(peers))
        if j < NB - 1:
            left.append(
                send(plain.at[j], from_next.at[j], left_send.at[j], left_recv.at[j], {"dp": previous})
            )
        else:
            for h in range(2):
                left.append(
                    send(
                        plain.at[j, :, pl.ds(h * HALF, HALF)],
                        from_next_half.at[h],
                        left_send.at[j + h],
                        left_recv.at[j + h],
                        {"dp": previous},
                    )
                )

    row_head = lax.broadcasted_iota(jnp.int32, (LROWS, LROWS), 0) // HD
    col_head = lax.broadcasted_iota(jnp.int32, (LROWS, LROWS), 1) // HD
    diagonal = (row_head == col_head).astype(F32)
    factors = []
    for layer in range(LAYERS):
        wide = jnp.concatenate([p_ref[pl.ds(layer * LROWS, LROWS), :]] * (LROWS // HD), axis=1)
        wide = (wide * diagonal).T
        high = wide.astype(BF16)
        factors.append((high, (wide - high.astype(F32)).astype(BF16)))
    right = {}
    for a in (3, 2, 1, 0):
        for layer in range(LAYERS):
            rows = pl.ds(layer * LROWS, LROWS)
            high = plain[a, rows, :]
            low = (gbuf[a, rows, :] - high.astype(F32)).astype(BF16)
            p_high, p_low = factors[layer]
            value = (
                jnp.dot(p_high, high, preferred_element_type=F32)
                + jnp.dot(p_low, high, preferred_element_type=F32)
                + jnp.dot(p_high, low, preferred_element_type=F32)
            )
            value = value.T.astype(BF16)
            for yy in range(NY):
                for cc in range(2):
                    scaled[cc, a, pl.ds(yy * PIECE, PIECE), pl.ds(layer * LROWS, LROWS)] = value[
                        (yy * 2 + cc) * PIECE : (yy * 2 + cc + 1) * PIECE
                    ]
        if a > 0:
            right[a] = send(
                scaled.at[:, a], from_prev.at[a - 1], right_send.at[a - 1], right_recv.at[a - 1], {"dp": following}
            )

    def columns_of(s, b):
        if b < NB:
            return plain[b]
        if b < 2 * NB - 1:
            return from_next[b - NB]
        return from_next_half[s - 4]

    core_copies, y_copies, far_copies = {}, {}, {}

    def compute(s):
        tiles, _ = STAGES[s]
        keep, outgoing, incoming, _, _ = stage_refs[s]
        index = 0
        while index < len(tiles):
            kind, a, b = tiles[index]
            count = 1
            if kind == "own":
                while index + count < len(tiles) and tiles[index + count] == ("own", a + count, b):
                    count += 1
            columns = columns_of(s, b) if kind == "own" else from_next[b]
            width = columns.shape[1]
            for which, ref in ((core, keep), (1 - core, outgoing)):
                if kind == "own":
                    lhs = scaled[which, a : a + count].reshape(count * HALF, ROWS)
                else:
                    lhs = from_prev[a - 1, which]
                product = jnp.dot(lhs, columns, preferred_element_type=F32)
                ref[index : index + count] = product.reshape(count, HALF, width).astype(ref.dtype)
            index += count
        core_copies[s] = send(outgoing, incoming, core_send.at[s], core_recv.at[s], {"head": other})

    def presum(s):
        tiles, width = STAGES[s]
        keep, _, incoming, pieces, arrived = stage_refs[s]
        core_copies[s].wait_recv()
        total = (keep[...] + incoming[...].astype(F32)).astype(BF16)
        for yy in range(NY):
            pieces[yy] = total[:, yy * PIECE : (yy + 1) * PIECE, :]
        y_copies[s] = []
        for d in range(1, NY):
            y_copies[s].append(
                send(
                    pieces.at[lax.rem(y + d, NY)],
                    arrived.at[d - 1],
                    y_send.at[s, d - 1],
                    y_recv.at[s, d - 1],
                    {"head": peers[d - 1]},
                )
            )

    def final(s):
        tiles, width = STAGES[s]
        keep, _, incoming, _, arrived = stage_refs[s]
        for copy in y_copies[s]:
            copy.wait_recv()
        mine = pl.ds(pl.multiple_of(y * PIECE, PIECE), PIECE)
        sent = 0
        for t, (kind, a, b) in enumerate(tiles):
            value = keep[t, mine, :] + incoming[t, mine, :].astype(F32)
            for d in range(NY - 1):
                value = value + arrived[d, t].astype(F32)
            if kind == "own":
                out_ref[:, b - a - 1, a, pl.ds(COLUMN0[s], width)] = value
            else:
                ships[s][sent] = value.astype(BF16)
                sent += 1
        if sent:
            far_copies[s] = send(ships[s], fars[s], far_send.at[s - 2], far_recv.at[s - 2], {"dp": previous})

    compute(0)
    presum(0)
    left[0].wait_recv()
    compute(1)
    presum(1)
    final(0)
    left[1].wait_recv()
    right[3].wait_recv()
    right[2].wait_recv()
    compute(2)
    presum(2)
    final(1)
    left[2].wait_recv()
    right[1].wait_recv()
    compute(3)
    presum(3)
    final(2)
    final(3)
    left[3].wait_recv()
    compute(4)
    presum(4)
    left[4].wait_recv()
    compute(5)
    presum(5)
    for s in (2, 3):
        far_copies[s].wait_recv()
        sent = 0
        for kind, a, c in STAGES[s][0]:
            if kind == "far":
                out_ref[:, 2 * NB + c - a - 1, a, :] = fars[s][sent].astype(F32)
                sent += 1
    final(4)
    final(5)
    for copy in pending:
        copy.wait_send()


def influence(gradients, preconditioner):
    scratch = [
        pltpu.VMEM((NB, ROWS, BS), F32),
        pltpu.VMEM((NB, ROWS, BS), BF16),
        pltpu.VMEM((2, NB, HALF, ROWS), BF16),
        pltpu.VMEM((NB - 1, ROWS, BS), BF16),
        pltpu.VMEM((2, ROWS, HALF), BF16),
        pltpu.VMEM((NB - 1, 2, HALF, ROWS), BF16),
        pltpu.VMEM((4, PIECE, BS), BF16),
        pltpu.VMEM((2, PIECE, BS), BF16),
        pltpu.VMEM((4, PIECE, BS), BF16),
        pltpu.VMEM((2, PIECE, BS), BF16),
    ]
    for tiles, width in STAGES:
        n = len(tiles)
        scratch += [
            pltpu.VMEM((n, HALF, width), F32),
            pltpu.VMEM((n, HALF, width), BF16),
            pltpu.VMEM((n, HALF, width), BF16),
            pltpu.VMEM((NY, n, PIECE, width), BF16),
            pltpu.VMEM((NY - 1, n, PIECE, width), BF16),
        ]
    dma = pltpu.SemaphoreType.DMA
    scratch += [
        dma((NB,)),
        dma((NB + 1,)),
        dma((NB + 1,)),
        dma((NB - 1,)),
        dma((NB - 1,)),
        dma((NSTAGE,)),
        dma((NSTAGE,)),
        dma((NSTAGE, NY - 1)),
        dma((NSTAGE, NY - 1)),
        dma((2,)),
        dma((2,)),
    ]
    return pl.pallas_call(
        kernel,
        out_shape=jax.ShapeDtypeStruct((PIECE, SLOTS, NB, BS), F32),
        in_specs=[pl.BlockSpec(memory_space=pltpu.HBM), pl.BlockSpec(memory_space=pltpu.VMEM)],
        out_specs=pl.BlockSpec(memory_space=pltpu.VMEM),
        scratch_shapes=scratch,
        compiler_params=pltpu.CompilerParams(
            collective_id=0, has_side_effects=True, vmem_limit_bytes=61 * 1024 * 1024
        ),
    )(gradients, preconditioner)


def per_device(gradients, preconditioner, partners):
    tiles = influence(gradients.reshape(ROWS, NB * BS), preconditioner.reshape(ROWS, HD))
    live = (partners >= 0).astype(F32)
    return (tiles * live.T[None, :, :, None]).transpose(0, 2, 1, 3)


def solution(mesh):
    in_specs = (P(None, "head", None, "dp"), P(None, "head", None, None), P("dp", None))
    out_specs = P("head", "dp", None, None)
    return jax.shard_map(
        per_device, mesh=mesh, in_specs=in_specs, out_specs=out_specs, check_vma=False
    )
```

```python
import jax
import jax.numpy as jnp
from jax import lax
from jax.experimental import pallas as pl
from jax.experimental.pallas import tpu as pltpu
from jax.sharding import PartitionSpec as P

MESH = pl.DeviceIdType.MESH
BF16 = jnp.bfloat16
F32 = jnp.float32

BS = 256
NB = 4
SLOTS = 7
ROWS = 768
LAYERS = 3
LROWS = ROWS // LAYERS
HD = 64
NY = 4
HALF = BS // 2
PIECE = HALF // NY
KH = ROWS // 2
LIVE_ROWS = 32
LANES = 128

STAGES = (
    tuple(("own", a, b) for b in range(1, NB) for a in range(b)),
    tuple(("fold", a, 0) for a in range(NB)),
    tuple(("fold", a, 1) for a in range(NB)),
    tuple(("fold", a, 2) for a in range(NB)),
    tuple(("fold", a, 3) for a in range(NB)) + (("far", 1, 0),),
    tuple(("far", 3, c) for c in range(3)) + tuple(("relay", 3, c) for c in range(3)),
    (("far", 2, 0), ("far", 2, 1)),
)
NSTAGE = len(STAGES)
ONE_BACK = ("fold", "far")
SHIP1 = [sum(kind in ONE_BACK for kind, _, _ in tiles) for tiles in STAGES]
RELAY_STAGE = 5
RX, RA2 = 4, 5


def kernel(g_hbm, p_ref, partners_ref, out_ref, *scratch):
    it = iter(scratch)
    take = lambda n: [next(it) for _ in range(n)]
    gbuf, plain, scaled, from_next, from_prev, left_mix, right_mix = take(7)
    live0, live1, live2 = take(3)
    ship2, got2 = take(2)
    stage_refs = [take(4) for _ in range(NSTAGE)]
    ship_refs = [take(2) if n else None for n in SHIP1]
    (load_sem, live_send, live_recv, left_send, left_recv, right_send, right_recv) = take(7)
    (core_send, core_recv, y_send, y_recv, ship_send, ship_recv) = take(6)

    n_dp = lax.axis_size("dp")
    dp = lax.axis_index("dp")
    head = lax.axis_index("head")
    core = lax.rem(head, 2)
    y = lax.div(head, 2)
    before, before2 = [lax.rem(dp + n_dp - d, n_dp) for d in (1, 2)]
    after, after2 = [lax.rem(dp + d, n_dp) for d in (1, 2)]
    other = head + 1 - 2 * core
    peers = [lax.rem(y + d, NY) * 2 + core for d in range(1, NY)]

    loads = {}
    for j in (0, 3, 1, 2):
        load = pltpu.make_async_copy(g_hbm.at[:, pl.ds(j * BS, BS)], gbuf.at[j], load_sem.at[j])
        load.start()
        loads[j] = load

    barrier = pltpu.get_barrier_semaphore()
    neighbours = (before, after, before2, after2)
    for target in neighbours:
        pl.semaphore_signal(barrier, inc=1, device_id={"dp": target}, device_id_type=MESH)
    for target in [other] + peers:
        pl.semaphore_signal(barrier, inc=1, device_id={"head": target}, device_id_type=MESH)

    pending = []

    def send(src, dst, send_sem, recv_sem, device):
        copy = pltpu.make_async_remote_copy(
            src_ref=src,
            dst_ref=dst,
            send_sem=send_sem,
            recv_sem=recv_sem,
            device_id=device,
            device_id_type=MESH,
        )
        copy.start()
        pending.append(copy)
        return copy

    live0[...] = jnp.zeros((LIVE_ROWS, LANES), F32)
    for a in range(NB):
        for k in range(SLOTS):
            slot = jnp.where(partners_ref[a, k] >= 0, 1.0, 0.0).astype(F32)
            live0[a * 8 + k : a * 8 + k + 1, :] = jnp.full((1, LANES), slot, F32)

    def live(ref, a, target, width=BS):
        row = a * 8 + target - a - 1
        return jnp.concatenate([ref[row : row + 1, :]] * (width // LANES), axis=1)

    def load_plain(j):
        loads[j].wait()
        plain[j] = gbuf[j].astype(BF16)

    left, right = {}, {}

    def send_left(n, src):
        left[n] = send(src, from_next.at[n], left_send.at[n], left_recv.at[n], {"dp": before})

    def send_right(n, src):
        right[n] = send(src, from_prev.at[n], right_send.at[n], right_recv.at[n], {"dp": after})

    a_rows, b_rows = pl.ds(0, KH), pl.ds(KH, KH)

    row_head = lax.broadcasted_iota(jnp.int32, (LROWS, LROWS), 0) // HD
    col_head = lax.broadcasted_iota(jnp.int32, (LROWS, LROWS), 1) // HD
    diagonal = (row_head == col_head).astype(F32)
    factors = []
    for layer in range(LAYERS):
        wide = jnp.concatenate([p_ref[pl.ds(layer * LROWS, LROWS), :]] * (LROWS // HD), axis=1)
        wide = (wide * diagonal).T
        high = wide.astype(BF16)
        factors.append((high, (wide - high.astype(F32)).astype(BF16)))

    def scale(a):
        for layer in range(LAYERS):
            rows = pl.ds(layer * LROWS, LROWS)
            high = plain[a, rows, :]
            low = (gbuf[a, rows, :] - high.astype(F32)).astype(BF16)
            p_high, p_low = factors[layer]
            value = (
                jnp.dot(p_high, high, preferred_element_type=F32)
                + jnp.dot(p_low, high, preferred_element_type=F32)
                + jnp.dot(p_high, low, preferred_element_type=F32)
            )
            value = value.T.astype(BF16)
            for yy in range(NY):
                for cc in range(2):
                    scaled[cc, a, pl.ds(yy * PIECE, PIECE), rows] = value[
                        (yy * 2 + cc) * PIECE : (yy * 2 + cc + 1) * PIECE
                    ]

    def either(flag, yes, no):
        return (flag * yes.astype(F32) + (1.0 - flag) * no.astype(F32)).astype(BF16)

    load_plain(0)
    pl.semaphore_wait(barrier, len(neighbours) + 1 + len(peers))
    send_left(0, plain.at[0, a_rows])
    live_copies = [
        send(live0, live1, live_send.at[0], live_recv.at[0], {"dp": after}),
        send(live0, live2, live_send.at[1], live_recv.at[1], {"dp": after2}),
    ]
    load_plain(3)
    scale(3)
    send_right(3, scaled.at[:, 3, :, b_rows])
    load_plain(1)
    send_left(1, plain.at[1, a_rows])
    scale(0)
    scale(1)
    reach = live(live0, 1, 8, KH)
    for cc in range(2):
        right_mix[0, cc] = either(reach, scaled[cc, 1, :, a_rows], scaled[cc, 0, :, b_rows])
    send_right(0, right_mix.at[0])
    send_right(1, scaled.at[:, 1, :, b_rows])
    load_plain(2)
    for copy in live_copies:
        copy.wait_recv()
    reach = live(live2, 2, 8)
    for n in (2, 3):
        left_mix[n - 2] = either(reach, plain[n - 2, b_rows, :], plain[n, a_rows, :])
        send_left(n, left_mix.at[n - 2])
    scale(2)
    send_right(2, scaled.at[:, 2, :, b_rows])

    core_copies, y_copies, ship_copies, ship2_copies = {}, {}, {}, {}

    def own_rows(a, count, columns):
        lhs = scaled[:, a : a + count, :, columns]
        return lhs.reshape(2 * count * HALF, lhs.shape[-1])

    def product(lhs, rhs):
        return jnp.dot(lhs, rhs, preferred_element_type=F32)

    def prev_rows(n):
        return from_prev[n].reshape(BS, KH)

    def compute(s):
        tiles = STAGES[s]
        tile, incoming, _, _ = stage_refs[s]
        if s == 0:
            index = 0
            for b in range(1, NB):
                value = product(own_rows(0, b, pl.ds(0, ROWS)), plain[b])
                tile[:, index : index + b] = value.reshape(2, b, HALF, BS).astype(BF16)
                index += b
        for index, (kind, a, n) in enumerate(tiles):
            if kind == "fold":
                if a == 0:
                    forward = product(own_rows(0, NB, a_rows), from_next[n]).reshape(2, NB, HALF, BS)
                value = forward[:, a] * live(live0, a, NB + n) + product(
                    prev_rows(n), plain[a, b_rows, :]
                ).reshape(2, HALF, BS) * live(live1, n, NB + a)
            elif kind == "far":
                value = product(prev_rows({1: 0, 2: RA2, 3: RX}[a]), from_next[n])
                if a < 3:
                    value = value + product(prev_rows(a), from_next[2 + n])
                value = value.reshape(2, HALF, BS) * live(live1, a, 2 * NB + n)
            elif kind == "relay":
                value = product(prev_rows(RX), plain[n, b_rows, :]).reshape(2, HALF, BS)
                value = value * live(live2, a, 2 * NB + n)
            if kind != "own":
                tile[:, index] = value.astype(BF16)
        core_copies[s] = send(tile.at[1 - core], incoming, core_send.at[s], core_recv.at[s], {"head": other})

    def presum(s):
        tile, incoming, pieces, arrived = stage_refs[s]
        core_copies[s].wait_recv()
        total = (tile[core].astype(F32) + incoming[...].astype(F32)).astype(BF16)
        for yy in range(NY):
            pieces[yy] = total[:, yy * PIECE : (yy + 1) * PIECE, :]
        y_copies[s] = [
            send(
                pieces.at[lax.rem(y + d, NY)],
                arrived.at[d - 1],
                y_send.at[s, d - 1],
                y_recv.at[s, d - 1],
                {"head": peers[d - 1]},
            )
            for d in range(1, NY)
        ]

    def final(s):
        tile, incoming, _, arrived = stage_refs[s]
        for copy in y_copies[s]:
            copy.wait_recv()
        mine = pl.ds(pl.multiple_of(y * PIECE, PIECE), PIECE)
        sent, sent2 = 0, 0
        for t, (kind, a, n) in enumerate(STAGES[s]):
            value = tile[core, t, mine, :].astype(F32) + incoming[t, mine, :].astype(F32)
            for d in range(NY - 1):
                value = value + arrived[d, t].astype(F32)
            if kind == "own":
                out_ref[:, n - a - 1, a, :] = value * live(live0, a, n)
            elif kind == "fold":
                out_ref[:, NB + n - a - 1, a, :] = value * live(live0, a, NB + n)
                ship_refs[s][0][sent] = (value * live(live1, n, NB + a)).astype(BF16)
                sent += 1
            elif kind == "far":
                ship_refs[s][0][sent] = value.astype(BF16)
                sent += 1
            else:
                ship2[sent2] = value.astype(BF16)
                sent2 += 1
        if sent2:
            ship2_copies[s] = send(ship2, got2, ship_send.at[NSTAGE], ship_recv.at[NSTAGE], {"dp": before2})
        if sent:
            ship_copies[s] = send(*ship_refs[s], ship_send.at[s], ship_recv.at[s], {"dp": before})

    def collect(s):
        if s in ship_copies:
            ship_copies[s].wait_recv()
        if s in ship2_copies:
            ship2_copies[s].wait_recv()
        got, got_far = 0, 0
        for kind, a, n in STAGES[s]:
            if kind == "fold":
                row, target = n, NB + a
                column = target - row - 1
                out_ref[:, column, row, :] = out_ref[:, column, row, :] + ship_refs[s][1][got].astype(F32)
                got += 1
            elif kind == "far":
                value = ship_refs[s][1][got].astype(F32)
                if a == 3:
                    value = value + got2[n].astype(F32)
                out_ref[:, 2 * NB + n - a - 1, a, :] = value
                got += 1

    compute(0)
    right[3].wait_recv()
    reach = live(live1, 3, 8, KH)
    for cc in range(2):
        right_mix[1, cc] = either(reach, from_prev[3, cc], scaled[cc, 3, :, a_rows])
    send_right(RX, right_mix.at[1])
    send_right(RA2, scaled.at[:, 2, :, a_rows])
    presum(0)
    left[0].wait_recv()
    right[0].wait_recv()
    compute(1)
    presum(1)
    final(0)
    left[1].wait_recv()
    right[1].wait_recv()
    compute(2)
    presum(2)
    final(1)
    left[2].wait_recv()
    right[2].wait_recv()
    compute(3)
    presum(3)
    final(2)
    left[3].wait_recv()
    compute(4)
    presum(4)
    final(3)
    right[RX].wait_recv()
    compute(5)
    presum(5)
    final(4)
    right[RA2].wait_recv()
    compute(6)
    presum(6)
    final(5)
    for s in range(1, 5):
        collect(s)
    final(6)
    collect(5)
    collect(6)
    for copy in pending:
        copy.wait_send()


def influence(gradients, preconditioner, partners):
    dma = pltpu.SemaphoreType.DMA
    scratch = [
        pltpu.VMEM((NB, ROWS, BS), F32),
        pltpu.VMEM((NB, ROWS, BS), BF16),
        pltpu.VMEM((2, NB, HALF, ROWS), BF16),
        pltpu.VMEM((NB, KH, BS), BF16),
        pltpu.VMEM((6, 2, HALF, KH), BF16),
        pltpu.VMEM((2, KH, BS), BF16),
        pltpu.VMEM((2, 2, HALF, KH), BF16),
        pltpu.VMEM((LIVE_ROWS, LANES), F32),
        pltpu.VMEM((LIVE_ROWS, LANES), F32),
        pltpu.VMEM((LIVE_ROWS, LANES), F32),
        pltpu.VMEM((3, PIECE, BS), BF16),
        pltpu.VMEM((3, PIECE, BS), BF16),
    ]
    for tiles in STAGES:
        n = len(tiles)
        scratch += [
            pltpu.VMEM((2, n, HALF, BS), BF16),
            pltpu.VMEM((n, HALF, BS), BF16),
            pltpu.VMEM((NY, n, PIECE, BS), BF16),
            pltpu.VMEM((NY - 1, n, PIECE, BS), BF16),
        ]
    for n in SHIP1:
        if n:
            scratch += [pltpu.VMEM((n, PIECE, BS), BF16)] * 2
    scratch += [
        dma((NB,)),
        dma((2,)),
        dma((2,)),
        dma((NB,)),
        dma((NB,)),
        dma((6,)),
        dma((6,)),
        dma((NSTAGE,)),
        dma((NSTAGE,)),
        dma((NSTAGE, NY - 1)),
        dma((NSTAGE, NY - 1)),
        dma((NSTAGE + 1,)),
        dma((NSTAGE + 1,)),
    ]
    return pl.pallas_call(
        kernel,
        out_shape=jax.ShapeDtypeStruct((PIECE, SLOTS, NB, BS), F32),
        in_specs=[
            pl.BlockSpec(memory_space=pltpu.HBM),
            pl.BlockSpec(memory_space=pltpu.VMEM),
            pl.BlockSpec(memory_space=pltpu.SMEM),
        ],
        out_specs=pl.BlockSpec(memory_space=pltpu.VMEM),
        scratch_shapes=scratch,
        compiler_params=pltpu.CompilerParams(
            collective_id=0, has_side_effects=True, vmem_limit_bytes=61 * 1024 * 1024
        ),
    )(gradients, preconditioner, partners)


def per_device(gradients, preconditioner, partners):
    tiles = influence(gradients.reshape(ROWS, NB * BS), preconditioner.reshape(ROWS, HD), partners)
    return tiles.transpose(0, 2, 1, 3)


def solution(mesh):
    in_specs = (P(None, "head", None, "dp"), P(None, "head", None, None), P("dp", None))
    out_specs = P("head", "dp", None, None)
    return jax.shard_map(
        per_device, mesh=mesh, in_specs=in_specs, out_specs=out_specs, check_vma=False
    )
```

```python
import jax
import jax.numpy as jnp
from jax import lax
from jax.experimental import pallas as pl
from jax.experimental.pallas import tpu as pltpu
from jax.sharding import PartitionSpec as P

MESH = pl.DeviceIdType.MESH
BF16 = jnp.bfloat16
F32 = jnp.float32

BS = 256
NB = 4
SLOTS = 7
ROWS = 768
LAYERS = 3
LROWS = ROWS // LAYERS
HD = 64
NY = 4
HALF = BS // 2
PIECE = HALF // NY
KH = ROWS // 2
LIVE_ROWS = 32
LANES = 128

def fold(n):
    return tuple((("alpha", a, n), ("beta", n, a)) for a in range(NB))


STAGES = (
    tuple((("own", a, b),) for b in range(1, NB) for a in range(min(b, 2))),
    fold(0),
    fold(3),
    (
        (("far", 3, 0), ("relay", 3, 0)),
        (("far", 3, 1), ("relay", 3, 1)),
        (("own", 2, 3), ("relay", 3, 2)),
    ),
    fold(1),
    fold(2),
    (
        (("far", 2, 0), ("far", 3, 2)),
        (("far", 2, 1), ("far", 1, 0)),
    ),
)
NSTAGE = len(STAGES)
ONE_BACK = ("beta", "far")


def ship_terms(slot):
    return [term for term in slot if term[0] in ONE_BACK]


SHIP1 = [sum(len(ship_terms(slot)) > 0 for slot in slots) for slots in STAGES]
RX, RA2 = 4, 5


def kernel(g_hbm, p_hbm, partners_hbm, out_ref, *scratch):
    it = iter(scratch)
    take = lambda n: [next(it) for _ in range(n)]
    gbuf, pbuf, partners_smem, plain, scaled, from_next, from_prev, left_mix, right_mix = take(9)
    live0, live1, live2 = take(3)
    ship2, got2 = take(2)
    stage_refs = [take(4) for _ in range(NSTAGE)]
    ship_refs = [take(2) if n else None for n in SHIP1]
    (load_sem, live_send, live_recv, left_send, left_recv, right_send, right_recv) = take(7)
    (core_send, core_recv, y_send, y_recv, ship_send, ship_recv) = take(6)

    n_dp = lax.axis_size("dp")
    dp = lax.axis_index("dp")
    head = lax.axis_index("head")
    core = lax.rem(head, 2)
    y = lax.div(head, 2)
    before, before2 = [lax.rem(dp + n_dp - d, n_dp) for d in (1, 2)]
    after, after2 = [lax.rem(dp + d, n_dp) for d in (1, 2)]
    other = head + 1 - 2 * core
    peers = [lax.rem(y + d, NY) * 2 + core for d in range(1, NY)]

    barrier = pltpu.get_barrier_semaphore()
    neighbours = (before, after, before2, after2)
    for target in neighbours:
        pl.semaphore_signal(barrier, inc=1, device_id={"dp": target}, device_id_type=MESH)
    for target in [other] + peers:
        pl.semaphore_signal(barrier, inc=1, device_id={"head": target}, device_id_type=MESH)

    loads = {}
    for name, src, dst in [("p", p_hbm, pbuf)] + [
        (j, g_hbm.at[:, pl.ds(j * BS, BS)], gbuf.at[j]) for j in (3, 0, 1, 2)
    ] + [("partners", partners_hbm, partners_smem)]:
        load = pltpu.make_async_copy(src, dst, load_sem.at[len(loads)])
        load.start()
        loads[name] = load

    pending = []

    def send(src, dst, send_sem, recv_sem, device):
        copy = pltpu.make_async_remote_copy(
            src_ref=src,
            dst_ref=dst,
            send_sem=send_sem,
            recv_sem=recv_sem,
            device_id=device,
            device_id_type=MESH,
        )
        copy.start()
        pending.append(copy)
        return copy

    def live(ref, a, target, width=BS):
        row = a * 8 + target - a - 1
        return jnp.concatenate([ref[row : row + 1, :]] * (width // LANES), axis=1)

    def load_plain(j):
        loads[j].wait()
        plain[j] = gbuf[j].astype(BF16)

    left, right = {}, {}

    def send_left(n, src):
        left[n] = send(src, from_next.at[n], left_send.at[n], left_recv.at[n], {"dp": before})

    def send_right(n, src):
        right[n] = send(src, from_prev.at[n], right_send.at[n], right_recv.at[n], {"dp": after})

    a_rows, b_rows = pl.ds(0, KH), pl.ds(KH, KH)

    def scale(a):
        for layer in range(LAYERS):
            rows = pl.ds(layer * LROWS, LROWS)
            high = plain[a, rows, :]
            low = (gbuf[a, rows, :] - high.astype(F32)).astype(BF16)
            p_high, p_low = factors[layer]
            value = (
                jnp.dot(p_high, high, preferred_element_type=F32)
                + jnp.dot(p_low, high, preferred_element_type=F32)
                + jnp.dot(p_high, low, preferred_element_type=F32)
            )
            value = value.T.astype(BF16)
            for yy in range(NY):
                for cc in range(2):
                    scaled[cc, a, pl.ds(yy * PIECE, PIECE), rows] = value[
                        (yy * 2 + cc) * PIECE : (yy * 2 + cc + 1) * PIECE
                    ]

    def either(flag, yes, no):
        return (flag * yes.astype(F32) + (1.0 - flag) * no.astype(F32)).astype(BF16)

    row_head = lax.broadcasted_iota(jnp.int32, (LROWS, LROWS), 0) // HD
    col_head = lax.broadcasted_iota(jnp.int32, (LROWS, LROWS), 1) // HD
    diagonal = (row_head == col_head).astype(F32)
    loads["p"].wait()
    factors = []
    for layer in range(LAYERS):
        wide = jnp.concatenate([pbuf[pl.ds(layer * LROWS, LROWS), :]] * (LROWS // HD), axis=1)
        wide = (wide * diagonal).T
        high = wide.astype(BF16)
        factors.append((high, (wide - high.astype(F32)).astype(BF16)))

    load_plain(3)
    scale(3)
    load_plain(0)
    loads["partners"].wait()
    live0[...] = jnp.zeros((LIVE_ROWS, LANES), F32)
    for a in range(NB):
        for k in range(SLOTS):
            slot = jnp.where(partners_smem[a, k] >= 0, 1.0, 0.0).astype(F32)
            live0[a * 8 + k : a * 8 + k + 1, :] = jnp.full((1, LANES), slot, F32)

    pl.semaphore_wait(barrier, len(neighbours) + 1 + len(peers))
    live_copies = [
        send(live0, live1, live_send.at[0], live_recv.at[0], {"dp": after}),
        send(live0, live2, live_send.at[1], live_recv.at[1], {"dp": after2}),
    ]
    send_right(3, scaled.at[:, 3, :, b_rows])
    send_left(0, plain.at[0, a_rows])
    load_plain(1)
    send_left(1, plain.at[1, a_rows])
    scale(0)
    scale(1)
    reach = live(live0, 1, 8, KH)
    for cc in range(2):
        right_mix[0, cc] = either(reach, scaled[cc, 1, :, a_rows], scaled[cc, 0, :, b_rows])
    send_right(0, right_mix.at[0])
    load_plain(2)
    for copy in live_copies:
        copy.wait_recv()
    reach = live(live2, 2, 8)
    for n in (3, 2):
        left_mix[n - 2] = either(reach, plain[n - 2, b_rows, :], plain[n, a_rows, :])
        send_left(n, left_mix.at[n - 2])
    scale(2)

    core_copies, y_copies, ship_copies, ship2_copies = {}, {}, {}, {}

    def own_rows(a, count, columns):
        lhs = scaled[:, a : a + count, :, columns]
        return lhs.reshape(2 * count * HALF, lhs.shape[-1])

    def product(lhs, rhs):
        return jnp.dot(lhs, rhs, preferred_element_type=F32)

    def prev_rows(n):
        return from_prev[n].reshape(BS, KH)

    def part(kind, a, n, forward):
        if kind == "own":
            return product(own_rows(a, 1, pl.ds(0, ROWS)), plain[n]).reshape(2, HALF, BS) * live(live0, a, n)
        if kind == "alpha":
            return forward[:, a] * live(live0, a, NB + n)
        if kind == "beta":
            value = product(prev_rows(a), plain[n, b_rows, :])
            return value.reshape(2, HALF, BS) * live(live1, a, NB + n)
        if kind == "relay":
            value = product(prev_rows(RX), plain[n, b_rows, :])
            return value.reshape(2, HALF, BS) * live(live2, a, 2 * NB + n)
        value = product(prev_rows({1: 0, 2: RA2, 3: RX}[a]), from_next[n])
        if a < 3:
            value = value + product(prev_rows(a), from_next[2 + n])
        return value.reshape(2, HALF, BS) * live(live1, a, 2 * NB + n)

    def compute(s):
        tile, incoming, _, _ = stage_refs[s]
        if s == 0:
            index = 0
            for b in range(1, NB):
                count = min(b, 2)
                value = product(own_rows(0, count, pl.ds(0, ROWS)), plain[b])
                tile[:, index : index + count] = value.reshape(2, count, HALF, BS).astype(BF16)
                index += count
        else:
            forward = None
            if STAGES[s][0][0][0] == "alpha":
                n = STAGES[s][0][0][2]
                forward = product(own_rows(0, NB, a_rows), from_next[n]).reshape(2, NB, HALF, BS)
            for index, slot in enumerate(STAGES[s]):
                value = part(*slot[0], forward)
                for term in slot[1:]:
                    value = value + part(*term, forward)
                tile[:, index] = value.astype(BF16)
        core_copies[s] = send(tile.at[1 - core], incoming, core_send.at[s], core_recv.at[s], {"head": other})

    def presum(s):
        tile, incoming, pieces, arrived = stage_refs[s]
        core_copies[s].wait_recv()
        total = (tile[core].astype(F32) + incoming[...].astype(F32)).astype(BF16)
        for yy in range(NY):
            pieces[yy] = total[:, yy * PIECE : (yy + 1) * PIECE, :]
        y_copies[s] = [
            send(
                pieces.at[lax.rem(y + d, NY)],
                arrived.at[d - 1],
                y_send.at[s, d - 1],
                y_recv.at[s, d - 1],
                {"head": peers[d - 1]},
            )
            for d in range(1, NY)
        ]

    def final(s):
        tile, incoming, _, arrived = stage_refs[s]
        for copy in y_copies[s]:
            copy.wait_recv()
        mine = pl.ds(pl.multiple_of(y * PIECE, PIECE), PIECE)
        sent, sent2 = 0, 0
        for t, slot in enumerate(STAGES[s]):
            value = tile[core, t, mine, :].astype(F32) + incoming[t, mine, :].astype(F32)
            for d in range(NY - 1):
                value = value + arrived[d, t].astype(F32)
            for kind, a, n in slot:
                if kind == "own":
                    out_ref[:, n - a - 1, a, :] = value * live(live0, a, n)
                elif kind == "alpha":
                    out_ref[:, NB + n - a - 1, a, :] = value * live(live0, a, NB + n)
                elif kind == "relay":
                    ship2[sent2] = (value * live(live2, a, 2 * NB + n)).astype(BF16)
                    sent2 += 1
            flag = None
            for kind, a, n in ship_terms(slot):
                one = live(live1, a, (NB if kind == "beta" else 2 * NB) + n)
                flag = one if flag is None else flag + one
            if flag is not None:
                ship_refs[s][0][sent] = (value * flag).astype(BF16)
                sent += 1
        if sent2:
            ship2_copies[s] = send(ship2, got2, ship_send.at[NSTAGE], ship_recv.at[NSTAGE], {"dp": before2})
        if sent:
            ship_copies[s] = send(*ship_refs[s], ship_send.at[s], ship_recv.at[s], {"dp": before})

    def collect(s):
        if s in ship_copies:
            ship_copies[s].wait_recv()
        if s in ship2_copies:
            ship2_copies[s].wait_recv()
        got = 0
        for slot in STAGES[s]:
            for kind, a, n in ship_terms(slot):
                value = ship_refs[s][1][got].astype(F32)
                if kind == "beta":
                    column = NB + n - a - 1
                    out_ref[:, column, a, :] = out_ref[:, column, a, :] + value
                else:
                    value = value * live(live0, a, 2 * NB + n)
                    if a == 3:
                        value = value + got2[n].astype(F32)
                    out_ref[:, 2 * NB + n - a - 1, a, :] = value
            got += len(ship_terms(slot)) > 0

    compute(0)
    right[3].wait_recv()
    reach = live(live1, 3, 8, KH)
    for cc in range(2):
        right_mix[1, cc] = either(reach, from_prev[3, cc], scaled[cc, 3, :, a_rows])
    send_right(RX, right_mix.at[1])
    send_right(1, scaled.at[:, 1, :, b_rows])
    send_right(2, scaled.at[:, 2, :, b_rows])
    send_right(RA2, scaled.at[:, 2, :, a_rows])
    presum(0)
    left[0].wait_recv()
    right[0].wait_recv()
    compute(1)
    presum(1)
    left[1].wait_recv()
    left[3].wait_recv()
    compute(2)
    presum(2)
    final(0)
    right[RX].wait_recv()
    compute(3)
    presum(3)
    final(1)
    left[2].wait_recv()
    right[1].wait_recv()
    compute(4)
    presum(4)
    final(2)
    right[2].wait_recv()
    compute(5)
    presum(5)
    final(3)
    right[RA2].wait_recv()
    compute(6)
    presum(6)
    final(4)
    final(5)
    for s in range(1, 4):
        collect(s)
    final(6)
    for s in range(4, NSTAGE):
        collect(s)
    for copy in pending:
        copy.wait_send()


def influence(gradients, preconditioner, partners):
    dma = pltpu.SemaphoreType.DMA
    scratch = [
        pltpu.VMEM((NB, ROWS, BS), F32),
        pltpu.VMEM((ROWS, HD), F32),
        pltpu.SMEM((NB, SLOTS), jnp.int32),
        pltpu.VMEM((NB, ROWS, BS), BF16),
        pltpu.VMEM((2, NB, HALF, ROWS), BF16),
        pltpu.VMEM((NB, KH, BS), BF16),
        pltpu.VMEM((6, 2, HALF, KH), BF16),
        pltpu.VMEM((2, KH, BS), BF16),
        pltpu.VMEM((2, 2, HALF, KH), BF16),
        pltpu.VMEM((LIVE_ROWS, LANES), F32),
        pltpu.VMEM((LIVE_ROWS, LANES), F32),
        pltpu.VMEM((LIVE_ROWS, LANES), F32),
        pltpu.VMEM((3, PIECE, BS), BF16),
        pltpu.VMEM((3, PIECE, BS), BF16),
    ]
    for tiles in STAGES:
        n = len(tiles)
        scratch += [
            pltpu.VMEM((2, n, HALF, BS), BF16),
            pltpu.VMEM((n, HALF, BS), BF16),
            pltpu.VMEM((NY, n, PIECE, BS), BF16),
            pltpu.VMEM((NY - 1, n, PIECE, BS), BF16),
        ]
    for n in SHIP1:
        if n:
            scratch += [pltpu.VMEM((n, PIECE, BS), BF16)] * 2
    scratch += [
        dma((NB + 2,)),
        dma((2,)),
        dma((2,)),
        dma((NB,)),
        dma((NB,)),
        dma((6,)),
        dma((6,)),
        dma((NSTAGE,)),
        dma((NSTAGE,)),
        dma((NSTAGE, NY - 1)),
        dma((NSTAGE, NY - 1)),
        dma((NSTAGE + 1,)),
        dma((NSTAGE + 1,)),
    ]
    return pl.pallas_call(
        kernel,
        out_shape=jax.ShapeDtypeStruct((PIECE, SLOTS, NB, BS), F32),
        in_specs=[pl.BlockSpec(memory_space=pltpu.HBM)] * 3,
        out_specs=pl.BlockSpec(memory_space=pltpu.VMEM),
        scratch_shapes=scratch,
        compiler_params=pltpu.CompilerParams(
            collective_id=0, has_side_effects=True, vmem_limit_bytes=48 * 1024 * 1024
        ),
    )(*[pltpu.with_memory_space_constraint(x, pltpu.HBM) for x in (gradients, preconditioner, partners)])


def per_device(gradients, preconditioner, partners):
    tiles = influence(gradients.reshape(ROWS, NB * BS), preconditioner.reshape(ROWS, HD), partners)
    return tiles.transpose(0, 2, 1, 3)


def solution(mesh):
    in_specs = (P(None, "head", None, "dp"), P(None, "head", None, None), P("dp", None))
    out_specs = P("head", "dp", None, None)
    return jax.shard_map(
        per_device, mesh=mesh, in_specs=in_specs, out_specs=out_specs, check_vma=False
    )
```

```python
import jax
import jax.numpy as jnp
from jax import lax
from jax.experimental import pallas as pl
from jax.experimental.pallas import tpu as pltpu
from jax.sharding import PartitionSpec as P

MESH = pl.DeviceIdType.MESH
BF16 = jnp.bfloat16
F32 = jnp.float32

BS = 256
NB = 4
SLOTS = 7
ROWS = 768
LAYERS = 3
LROWS = ROWS // LAYERS
HD = 64
NY = 4
HALF = BS // 2
PIECE = HALF // NY
KH = ROWS // 2
LIVE_ROWS = 32
LANES = 128

def fold(n):
    return tuple((("alpha", a, n), ("beta", n, a)) for a in range(NB))


STAGES = (
    tuple((("own", a, b),) for a, b in ((0, 1), (0, 2), (1, 2), (1, 3), (2, 3))),
    fold(0),
    fold(3),
    fold(1),
    fold(2),
    (
        (("far", 3, 1), ("relay", 3, 0)),
        (("far", 3, 2), ("relay", 3, 1), ("far", 2, 0)),
        (("relay", 3, 2), ("far", 2, 1), ("far", 1, 0)),
    ),
    ((("ahead", 1, 0),), (("ahead", 2, 0),), (("ahead", 3, 0), ("own", 0, 3))),
)
NSTAGE = len(STAGES)
ONE_BACK = ("beta", "far")


def ship_terms(slot):
    return [term for term in slot if term[0] in ONE_BACK]


SHIP1 = [sum(len(ship_terms(slot)) > 0 for slot in slots) for slots in STAGES]
RX = LX = 4
MIXED = 5


def kernel(g_hbm, p_hbm, partners_hbm, out_ref, *scratch):
    it = iter(scratch)
    take = lambda n: [next(it) for _ in range(n)]
    gbuf, pbuf, partners_smem, plain, scaled, from_next, from_prev, left_mix, right_mix, early = take(10)
    live0, live1, live2 = take(3)
    ship2, got2 = take(2)
    stage_refs = [take(4) for _ in range(NSTAGE)]
    ship_refs = [take(2) if n else None for n in SHIP1]
    (load_sem, live_send, live_recv, left_send, left_recv, right_send, right_recv) = take(7)
    (core_send, core_recv, y_send, y_recv, ship_send, ship_recv) = take(6)

    n_dp = lax.axis_size("dp")
    dp = lax.axis_index("dp")
    head = lax.axis_index("head")
    core = lax.rem(head, 2)
    y = lax.div(head, 2)
    before, before2 = [lax.rem(dp + n_dp - d, n_dp) for d in (1, 2)]
    after, after2 = [lax.rem(dp + d, n_dp) for d in (1, 2)]
    other = head + 1 - 2 * core
    peers = [lax.rem(y + d, NY) * 2 + core for d in range(1, NY)]

    barrier = pltpu.get_barrier_semaphore()
    neighbours = (before, after, before2, after2)
    for target in neighbours:
        pl.semaphore_signal(barrier, inc=1, device_id={"dp": target}, device_id_type=MESH)
    for target in [other] + peers:
        pl.semaphore_signal(barrier, inc=1, device_id={"head": target}, device_id_type=MESH)

    loads = {}
    blocks = [(j, g_hbm.at[:, pl.ds(j * BS, BS)], gbuf.at[j]) for j in (0, 2, 3, 1)]
    tables = [("partners", partners_hbm, partners_smem), ("p", p_hbm, pbuf)]
    for name, src, dst in tables + blocks:
        load = pltpu.make_async_copy(src, dst, load_sem.at[len(loads)])
        load.start()
        loads[name] = load

    pending = []

    def send(src, dst, send_sem, recv_sem, device):
        copy = pltpu.make_async_remote_copy(
            src_ref=src,
            dst_ref=dst,
            send_sem=send_sem,
            recv_sem=recv_sem,
            device_id=device,
            device_id_type=MESH,
        )
        copy.start()
        pending.append(copy)
        return copy

    def live(ref, a, target, width=BS):
        row = a * 8 + target - a - 1
        return jnp.concatenate([ref[row : row + 1, :]] * (width // LANES), axis=1)

    def load_plain(j):
        loads[j].wait()
        plain[j] = gbuf[j].astype(BF16)

    left, right = {}, {}

    def send_left(n, src):
        left[n] = send(src, from_next.at[n], left_send.at[n], left_recv.at[n], {"dp": before})

    def send_right(n, src, dst=None):
        dst = from_prev.at[n] if dst is None else dst
        right[n] = send(src, dst, right_send.at[n], right_recv.at[n], {"dp": after})

    a_rows, b_rows = pl.ds(0, KH), pl.ds(KH, KH)

    def scale(a, layers=range(LAYERS)):
        for layer in layers:
            rows = pl.ds(layer * LROWS, LROWS)
            high = plain[a, rows, :]
            low = (gbuf[a, rows, :] - high.astype(F32)).astype(BF16)
            p_high, p_low = factors[layer]
            value = (
                jnp.dot(p_high, high, preferred_element_type=F32)
                + jnp.dot(p_low, high, preferred_element_type=F32)
                + jnp.dot(p_high, low, preferred_element_type=F32)
            )
            value = value.T.astype(BF16)
            for yy in range(NY):
                for cc in range(2):
                    scaled[cc, a, pl.ds(yy * PIECE, PIECE), rows] = value[
                        (yy * 2 + cc) * PIECE : (yy * 2 + cc + 1) * PIECE
                    ]

    def either(flag, yes, no):
        return (flag * yes.astype(F32) + (1.0 - flag) * no.astype(F32)).astype(BF16)

    row_head = lax.broadcasted_iota(jnp.int32, (LROWS, LROWS), 0) // HD
    col_head = lax.broadcasted_iota(jnp.int32, (LROWS, LROWS), 1) // HD
    diagonal = (row_head == col_head).astype(F32)
    loads["p"].wait()
    factors = []
    for layer in range(LAYERS):
        wide = jnp.concatenate([pbuf[pl.ds(layer * LROWS, LROWS), :]] * (LROWS // HD), axis=1)
        wide = (wide * diagonal).T
        high = wide.astype(BF16)
        factors.append((high, (wide - high.astype(F32)).astype(BF16)))

    loads["partners"].wait()
    live0[...] = jnp.zeros((LIVE_ROWS, LANES), F32)
    for a in range(NB):
        for k in range(SLOTS):
            slot = jnp.where(partners_smem[a, k] >= 0, 1.0, 0.0).astype(F32)
            live0[a * 8 + k : a * 8 + k + 1, :] = jnp.full((1, LANES), slot, F32)

    load_plain(0)
    scale(0, (1, 2))
    load_plain(2)
    scale(2, (0, 1))
    reach = live(live0, 2, 9, KH)
    for cc in range(2):
        right_mix[0, cc] = either(reach, scaled[cc, 2, :, a_rows], scaled[cc, 0, :, b_rows])

    pl.semaphore_wait(barrier, len(neighbours) + 1 + len(peers))
    live_copies = [
        send(live0, live1, live_send.at[0], live_recv.at[0], {"dp": after}),
        send(live0, live2, live_send.at[1], live_recv.at[1], {"dp": after2}),
    ]
    send_right(0, right_mix.at[0])
    send_left(0, plain.at[0, a_rows])
    load_plain(3)
    scale(3, (1, 2))
    send_right(3, scaled.at[:, 3, :, b_rows])
    load_plain(1)
    scale(0, (0,))
    scale(2, (2,))
    scale(3, (0,))
    for copy in live_copies:
        copy.wait_recv()
    reach = live(live2, 2, 8)
    for n in (3, 2):
        left_mix[n - 2] = either(reach, plain[n - 2, b_rows, :], plain[n, a_rows, :])
    send_left(3, left_mix.at[1])
    send_left(1, plain.at[1, a_rows])
    send_left(2, left_mix.at[0])
    scale(1)
    send_right(1, scaled.at[:, 1, :, b_rows])
    send_right(2, scaled.at[:, 2, :, b_rows])

    core_copies, y_copies, ship_copies, ship2_copies = {}, {}, {}, {}

    def own_rows(a, count, columns):
        lhs = scaled[:, a : a + count, :, columns]
        return lhs.reshape(2 * count * HALF, lhs.shape[-1])

    def product(lhs, rhs):
        return jnp.dot(lhs, rhs, preferred_element_type=F32)

    def prev_rows(n):
        return from_prev[n].reshape(BS, KH)

    def flag_of(kind, a, n):
        if kind == "relay":
            return live(live2, a, 2 * NB + n)
        if kind in ONE_BACK:
            return live(live1, a, (NB if kind == "beta" else 2 * NB) + n)
        return live(live0, a, {"own": 0, "alpha": NB, "ahead": 2 * NB}[kind] + n)

    def beta(a, n):
        return product(prev_rows(a), plain[n, b_rows, :]).reshape(2, HALF, BS) * flag_of("beta", a, n)

    def far(a, n):
        value = product(prev_rows(a), from_next[2 + n])
        if n == 1:
            value = value + product(prev_rows(0), from_next[n])
        return value.reshape(2, HALF, BS) * flag_of("far", a, n)

    def mixed_early():
        early[:, 0] = far(2, 0)
        early[:, 1] = far(2, 1) + far(1, 0)

    def mixed(half):
        tile = stage_refs[MIXED][0]
        lhs = from_prev[RX, half]
        for index, (c, n) in enumerate(((1, 0), (2, 1), (None, 2))):
            value = product(lhs, plain[n, b_rows, :]) * flag_of("relay", 3, n)
            if c is not None:
                value = value + product(lhs, from_next[c]) * flag_of("far", 3, c)
            if index:
                value = value + early[half, index - 1]
            tile[half, index] = value.astype(BF16)

    def to_core(s):
        tile, incoming, _, _ = stage_refs[s]
        core_copies[s] = send(tile.at[1 - core], incoming, core_send.at[s], core_recv.at[s], {"head": other})

    def compute(s):
        tile = stage_refs[s][0]
        kind, _, n = STAGES[s][0][0]
        if kind == "own":
            index = 0
            for b, first, count in ((1, 0, 1), (2, 0, 2), (3, 1, 2)):
                value = product(own_rows(first, count, pl.ds(0, ROWS)), plain[b])
                tile[:, index : index + count] = value.reshape(2, count, HALF, BS).astype(BF16)
                index += count
        elif kind == "ahead":
            value = product(own_rows(1, NB - 1, a_rows), from_next[LX]).reshape(2, NB - 1, HALF, BS)
            tile[:, 0:2] = value[:, 0:2].astype(BF16)
            last = product(own_rows(0, 1, pl.ds(0, ROWS)), plain[3]).reshape(2, HALF, BS)
            last = last * flag_of("own", 0, 3) + value[:, 2] * flag_of("ahead", 3, 0)
            tile[:, 2] = last.astype(BF16)
        else:
            forward = product(own_rows(0, NB, a_rows), from_next[n]).reshape(2, NB, HALF, BS)
            for a in range(NB):
                tile[:, a] = (forward[:, a] * flag_of("alpha", a, n) + beta(n, a)).astype(BF16)
        to_core(s)

    def presum(s):
        tile, incoming, pieces, arrived = stage_refs[s]
        core_copies[s].wait_recv()
        total = (tile[core].astype(F32) + incoming[...].astype(F32)).astype(BF16)
        for yy in range(NY):
            pieces[yy] = total[:, yy * PIECE : (yy + 1) * PIECE, :]
        y_copies[s] = [
            send(
                pieces.at[lax.rem(y + d, NY)],
                arrived.at[d - 1],
                y_send.at[s, d - 1],
                y_recv.at[s, d - 1],
                {"head": peers[d - 1]},
            )
            for d in range(1, NY)
        ]

    def final(s):
        tile, incoming, _, arrived = stage_refs[s]
        for copy in y_copies[s]:
            copy.wait_recv()
        mine = pl.ds(pl.multiple_of(y * PIECE, PIECE), PIECE)
        sent, sent2 = 0, 0
        for t, slot in enumerate(STAGES[s]):
            value = tile[core, t, mine, :].astype(F32) + incoming[t, mine, :].astype(F32)
            for d in range(NY - 1):
                value = value + arrived[d, t].astype(F32)
            flag = None
            for term in slot:
                kind, a, n = term
                one = flag_of(*term)
                if kind in ONE_BACK:
                    flag = one if flag is None else flag + one
                elif kind == "relay":
                    ship2[n] = (value * one).astype(BF16)
                    sent2 += 1
                else:
                    target = {"own": 0, "alpha": NB, "ahead": 2 * NB}[kind] + n
                    out_ref[:, target - a - 1, a, :] = value * one
            if flag is not None:
                ship_refs[s][0][sent] = (value * flag).astype(BF16)
                sent += 1
        if sent2:
            ship2_copies[s] = send(ship2, got2, ship_send.at[NSTAGE], ship_recv.at[NSTAGE], {"dp": before2})
        if sent:
            ship_copies[s] = send(*ship_refs[s], ship_send.at[s], ship_recv.at[s], {"dp": before})

    def collect(s):
        if s in ship_copies:
            ship_copies[s].wait_recv()
        if s in ship2_copies:
            ship2_copies[s].wait_recv()
        got = 0
        for slot in STAGES[s]:
            for kind, a, n in ship_terms(slot):
                value = ship_refs[s][1][got].astype(F32)
                target = (NB if kind == "beta" else 2 * NB) + n
                if kind == "far":
                    value = value * live(live0, a, target)
                if kind == "beta" or n == 0:
                    value = value + out_ref[:, target - a - 1, a, :]
                elif a == 3:
                    value = value + got2[n].astype(F32)
                out_ref[:, target - a - 1, a, :] = value
            got += len(ship_terms(slot)) > 0
        if s in ship2_copies:
            out_ref[:, 2 * NB - 4, 3, :] = out_ref[:, 2 * NB - 4, 3, :] + got2[0].astype(F32)

    compute(0)
    presum(0)
    left[0].wait_recv()
    send_left(LX, from_next.at[0])
    right[0].wait_recv()
    compute(1)
    presum(1)
    right[3].wait_recv()
    reach = live(live1, 3, 8, KH)
    for cc in range(2):
        right_mix[1, cc] = either(reach, from_prev[3, cc], scaled[cc, 3, :, a_rows])
    send_right(RX, right_mix.at[1, 1 - core], from_prev.at[RX, 1 - core])
    send_right(RX + 1, right_mix.at[1, core], from_prev.at[RX, core])
    left[3].wait_recv()
    compute(2)
    presum(2)
    final(0)
    left[1].wait_recv()
    right[1].wait_recv()
    compute(3)
    presum(3)
    final(1)
    left[2].wait_recv()
    right[2].wait_recv()
    compute(4)
    mixed_early()
    presum(4)
    final(2)
    right[RX].wait_recv()
    mixed(1 - core)
    to_core(MIXED)
    final(3)
    right[RX + 1].wait_recv()
    mixed(core)
    presum(5)
    left[LX].wait_recv()
    compute(6)
    presum(6)
    final(4)
    collect(1)
    collect(2)
    final(5)
    collect(3)
    final(6)
    collect(4)
    collect(5)
    for copy in pending:
        copy.wait_send()


def influence(gradients, preconditioner, partners):
    dma = pltpu.SemaphoreType.DMA
    scratch = [
        pltpu.VMEM((NB, ROWS, BS), F32),
        pltpu.VMEM((ROWS, HD), F32),
        pltpu.SMEM((NB, SLOTS), jnp.int32),
        pltpu.VMEM((NB, ROWS, BS), BF16),
        pltpu.VMEM((2, NB, HALF, ROWS), BF16),
        pltpu.VMEM((NB + 1, KH, BS), BF16),
        pltpu.VMEM((NB + 1, 2, HALF, KH), BF16),
        pltpu.VMEM((2, KH, BS), BF16),
        pltpu.VMEM((2, 2, HALF, KH), BF16),
        pltpu.VMEM((2, 2, HALF, BS), F32),
        pltpu.VMEM((LIVE_ROWS, LANES), F32),
        pltpu.VMEM((LIVE_ROWS, LANES), F32),
        pltpu.VMEM((LIVE_ROWS, LANES), F32),
        pltpu.VMEM((3, PIECE, BS), BF16),
        pltpu.VMEM((3, PIECE, BS), BF16),
    ]
    for tiles in STAGES:
        n = len(tiles)
        scratch += [
            pltpu.VMEM((2, n, HALF, BS), BF16),
            pltpu.VMEM((n, HALF, BS), BF16),
            pltpu.VMEM((NY, n, PIECE, BS), BF16),
            pltpu.VMEM((NY - 1, n, PIECE, BS), BF16),
        ]
    for n in SHIP1:
        if n:
            scratch += [pltpu.VMEM((n, PIECE, BS), BF16)] * 2
    scratch += [
        dma((NB + 2,)),
        dma((2,)),
        dma((2,)),
        dma((NB + 1,)),
        dma((NB + 1,)),
        dma((NB + 2,)),
        dma((NB + 2,)),
        dma((NSTAGE,)),
        dma((NSTAGE,)),
        dma((NSTAGE, NY - 1)),
        dma((NSTAGE, NY - 1)),
        dma((NSTAGE + 1,)),
        dma((NSTAGE + 1,)),
    ]
    return pl.pallas_call(
        kernel,
        out_shape=jax.ShapeDtypeStruct((PIECE, SLOTS, NB, BS), F32),
        in_specs=[pl.BlockSpec(memory_space=pltpu.HBM)] * 3,
        out_specs=pl.BlockSpec(memory_space=pltpu.VMEM),
        scratch_shapes=scratch,
        compiler_params=pltpu.CompilerParams(
            collective_id=0, has_side_effects=True, vmem_limit_bytes=48 * 1024 * 1024
        ),
    )(*[pltpu.with_memory_space_constraint(x, pltpu.HBM) for x in (gradients, preconditioner, partners)])


def per_device(gradients, preconditioner, partners):
    tiles = influence(gradients.reshape(ROWS, NB * BS), preconditioner.reshape(ROWS, HD), partners)
    return tiles.transpose(0, 2, 1, 3)


def solution(mesh):
    in_specs = (P(None, "head", None, "dp"), P(None, "head", None, None), P("dp", None))
    out_specs = P("head", "dp", None, None)
    return jax.shard_map(
        per_device, mesh=mesh, in_specs=in_specs, out_specs=out_specs, check_vma=False
    )
```

```python
import jax
import jax.numpy as jnp
from jax import lax
from jax.experimental import pallas as pl
from jax.experimental.pallas import tpu as pltpu
from jax.sharding import PartitionSpec as P

MESH = pl.DeviceIdType.MESH
BF16 = jnp.bfloat16
F32 = jnp.float32

BS = 256
NB = 4
SLOTS = 7
ROWS = 768
LAYERS = 3
LROWS = ROWS // LAYERS
HD = 64
NY = 4
HALF = BS // 2
PIECE = HALF // NY
KH = ROWS // 2
LIVE_ROWS = 32
LANES = 128

def fold(n):
    return tuple((("alpha", a, n), ("beta", n, a)) for a in range(NB))


STAGES = (
    tuple((("own", a, b),) for a, b in ((0, 1), (0, 2), (1, 2), (1, 3), (2, 3))),
    fold(0),
    fold(3),
    fold(1),
    fold(2),
    (
        (("far", 3, 1), ("relay", 3, 0)),
        (("far", 3, 2), ("relay", 3, 1), ("far", 2, 0)),
        (("relay", 3, 2), ("far", 2, 1), ("far", 1, 0)),
    ),
    ((("ahead", 1, 0),), (("ahead", 2, 0),), (("ahead", 3, 0), ("own", 0, 3))),
)
NSTAGE = len(STAGES)
ONE_BACK = ("beta", "far")


def ship_terms(slot):
    return [term for term in slot if term[0] in ONE_BACK]


SHIP1 = [sum(len(ship_terms(slot)) > 0 for slot in slots) for slots in STAGES]
RX = LX = 4
MIXED = 5


def kernel(g_hbm, p_hbm, partners_hbm, out_ref, *scratch):
    it = iter(scratch)
    take = lambda n: [next(it) for _ in range(n)]
    gbuf, pbuf, partners_smem, plain, scaled, from_next, from_prev, left_mix, right_mix, early = take(10)
    live0, live1, live2 = take(3)
    ship2, got2 = take(2)
    stage_refs = [take(4) for _ in range(NSTAGE)]
    ship_refs = [take(2) if n else None for n in SHIP1]
    (load_sem, live_send, live_recv, left_send, left_recv, right_send, right_recv) = take(7)
    (core_send, core_recv, y_send, y_recv, ship_send, ship_recv) = take(6)

    n_dp = lax.axis_size("dp")
    dp = lax.axis_index("dp")
    head = lax.axis_index("head")
    core = lax.rem(head, 2)
    y = lax.div(head, 2)
    before, before2 = [lax.rem(dp + n_dp - d, n_dp) for d in (1, 2)]
    after, after2 = [lax.rem(dp + d, n_dp) for d in (1, 2)]
    other = head + 1 - 2 * core
    peers = [lax.rem(y + d, NY) * 2 + core for d in range(1, NY)]

    barrier = pltpu.get_barrier_semaphore()
    neighbours = (before, after, before2, after2)
    for target in neighbours:
        pl.semaphore_signal(barrier, inc=1, device_id={"dp": target}, device_id_type=MESH)
    for target in [other] + peers:
        pl.semaphore_signal(barrier, inc=1, device_id={"head": target}, device_id_type=MESH)

    loads = {}
    blocks = [(j, g_hbm.at[:, pl.ds(j * BS, BS)], gbuf.at[j]) for j in (0, 2, 3, 1)]
    tables = [("partners", partners_hbm, partners_smem), ("p", p_hbm, pbuf)]
    for name, src, dst in tables + blocks:
        load = pltpu.make_async_copy(src, dst, load_sem.at[len(loads)])
        load.start()
        loads[name] = load

    pending = []

    def send(src, dst, send_sem, recv_sem, device):
        copy = pltpu.make_async_remote_copy(
            src_ref=src,
            dst_ref=dst,
            send_sem=send_sem,
            recv_sem=recv_sem,
            device_id=device,
            device_id_type=MESH,
        )
        copy.start()
        pending.append(copy)
        return copy

    def live(ref, a, target, width=BS):
        row = a * 8 + target - a - 1
        return jnp.concatenate([ref[row : row + 1, :]] * (width // LANES), axis=1)

    def load_plain(j):
        loads[j].wait()
        plain[j] = gbuf[j].astype(BF16)

    left, right = {}, {}

    def send_left(n, src):
        left[n] = send(src, from_next.at[n], left_send.at[n], left_recv.at[n], {"dp": before})

    def send_right(n, src, dst=None):
        dst = from_prev.at[n] if dst is None else dst
        right[n] = send(src, dst, right_send.at[n], right_recv.at[n], {"dp": after})

    a_rows, b_rows = pl.ds(0, KH), pl.ds(KH, KH)

    def scale(a, layers=range(LAYERS)):
        for layer in layers:
            rows = pl.ds(layer * LROWS, LROWS)
            high = plain[a, rows, :]
            low = (gbuf[a, rows, :] - high.astype(F32)).astype(BF16)
            p_high, p_low = factors[layer]
            value = (
                jnp.dot(p_high, high, preferred_element_type=F32)
                + jnp.dot(p_low, high, preferred_element_type=F32)
                + jnp.dot(p_high, low, preferred_element_type=F32)
            )
            value = value.T.astype(BF16)
            for yy in range(NY):
                for cc in range(2):
                    scaled[cc, a, pl.ds(yy * PIECE, PIECE), rows] = value[
                        (yy * 2 + cc) * PIECE : (yy * 2 + cc + 1) * PIECE
                    ]

    def either(flag, yes, no):
        return (flag * yes.astype(F32) + (1.0 - flag) * no.astype(F32)).astype(BF16)

    row_head = lax.broadcasted_iota(jnp.int32, (LROWS, LROWS), 0) // HD
    col_head = lax.broadcasted_iota(jnp.int32, (LROWS, LROWS), 1) // HD
    diagonal = (row_head == col_head).astype(F32)
    loads["p"].wait()
    factors = []
    for layer in range(LAYERS):
        wide = jnp.concatenate([pbuf[pl.ds(layer * LROWS, LROWS), :]] * (LROWS // HD), axis=1)
        wide = (wide * diagonal).T
        high = wide.astype(BF16)
        factors.append((high, (wide - high.astype(F32)).astype(BF16)))

    loads["partners"].wait()
    live0[...] = jnp.zeros((LIVE_ROWS, LANES), F32)
    for a in range(NB):
        for k in range(SLOTS):
            slot = jnp.where(partners_smem[a, k] >= 0, 1.0, 0.0).astype(F32)
            live0[a * 8 + k : a * 8 + k + 1, :] = jnp.full((1, LANES), slot, F32)

    load_plain(0)
    scale(0, (1, 2))
    load_plain(2)
    scale(2, (0, 1))
    reach = live(live0, 2, 9, KH)
    for cc in range(2):
        right_mix[0, cc] = either(reach, scaled[cc, 2, :, a_rows], scaled[cc, 0, :, b_rows])

    pl.semaphore_wait(barrier, len(neighbours) + 1 + len(peers))
    live_copies = [
        send(live0, live1, live_send.at[0], live_recv.at[0], {"dp": after}),
        send(live0, live2, live_send.at[1], live_recv.at[1], {"dp": after2}),
    ]
    send_right(0, right_mix.at[0])
    send_left(0, plain.at[0, a_rows])
    load_plain(3)
    scale(3, (1, 2))
    send_right(3, scaled.at[:, 3, :, b_rows])
    load_plain(1)
    scale(0, (0,))
    scale(2, (2,))
    scale(3, (0,))
    for copy in live_copies:
        copy.wait_recv()
    reach = live(live2, 2, 8)
    for n in (3, 2):
        left_mix[n - 2] = either(reach, plain[n - 2, b_rows, :], plain[n, a_rows, :])
    send_left(3, left_mix.at[1])
    send_left(1, plain.at[1, a_rows])
    send_left(2, left_mix.at[0])
    scale(1)
    send_right(1, scaled.at[:, 1, :, b_rows])
    send_right(2, scaled.at[:, 2, :, b_rows])

    core_copies, y_copies, ship_copies, ship2_copies = {}, {}, {}, {}

    def own_rows(a, count, columns):
        lhs = scaled[:, a : a + count, :, columns]
        return lhs.reshape(2 * count * HALF, lhs.shape[-1])

    def product(lhs, rhs):
        return jnp.dot(lhs, rhs, preferred_element_type=F32)

    def prev_rows(n):
        return from_prev[n].reshape(BS, KH)

    def flag_of(kind, a, n):
        if kind == "relay":
            return live(live2, a, 2 * NB + n)
        if kind in ONE_BACK:
            return live(live1, a, (NB if kind == "beta" else 2 * NB) + n)
        return live(live0, a, {"own": 0, "alpha": NB, "ahead": 2 * NB}[kind] + n)

    def beta(a, n):
        return product(prev_rows(a), plain[n, b_rows, :]).reshape(2, HALF, BS) * flag_of("beta", a, n)

    def far(a, n):
        value = product(prev_rows(a), from_next[2 + n])
        if n == 1:
            value = value + product(prev_rows(0), from_next[n])
        return value.reshape(2, HALF, BS) * flag_of("far", a, n)

    def mixed_early():
        early[:, 0] = far(2, 0)
        early[:, 1] = far(2, 1) + far(1, 0)

    def mixed(half):
        tile = stage_refs[MIXED][0]
        lhs = from_prev[RX, half]
        for index, (c, n) in enumerate(((1, 0), (2, 1), (None, 2))):
            value = product(lhs, plain[n, b_rows, :]) * flag_of("relay", 3, n)
            if c is not None:
                value = value + product(lhs, from_next[c]) * flag_of("far", 3, c)
            if index:
                value = value + early[half, index - 1]
            tile[half, index] = value.astype(BF16)

    def to_core(s):
        tile, incoming, _, _ = stage_refs[s]
        core_copies[s] = send(tile.at[1 - core], incoming, core_send.at[s], core_recv.at[s], {"head": other})

    def compute(s):
        tile = stage_refs[s][0]
        kind, _, n = STAGES[s][0][0]
        if kind == "own":
            index = 0
            for b, first, count in ((1, 0, 1), (2, 0, 2), (3, 1, 2)):
                value = product(own_rows(first, count, pl.ds(0, ROWS)), plain[b])
                tile[:, index : index + count] = value.reshape(2, count, HALF, BS).astype(BF16)
                index += count
        elif kind == "ahead":
            value = product(own_rows(1, NB - 1, a_rows), from_next[LX]).reshape(2, NB - 1, HALF, BS)
            tile[:, 0:2] = value[:, 0:2].astype(BF16)
            last = product(own_rows(0, 1, pl.ds(0, ROWS)), plain[3]).reshape(2, HALF, BS)
            last = last * flag_of("own", 0, 3) + value[:, 2] * flag_of("ahead", 3, 0)
            tile[:, 2] = last.astype(BF16)
        else:
            forward = product(own_rows(0, NB, a_rows), from_next[n]).reshape(2, NB, HALF, BS)
            for a in range(NB):
                tile[:, a] = (forward[:, a] * flag_of("alpha", a, n) + beta(n, a)).astype(BF16)
        to_core(s)

    def presum(s):
        tile, incoming, pieces, arrived = stage_refs[s]
        core_copies[s].wait_recv()
        total = (tile[core].astype(F32) + incoming[...].astype(F32)).astype(BF16)
        for yy in range(NY):
            pieces[yy] = total[:, yy * PIECE : (yy + 1) * PIECE, :]
        y_copies[s] = [
            send(
                pieces.at[lax.rem(y + d, NY)],
                arrived.at[d - 1],
                y_send.at[s, d - 1],
                y_recv.at[s, d - 1],
                {"head": peers[d - 1]},
            )
            for d in range(1, NY)
        ]

    def final(s):
        tile, incoming, _, arrived = stage_refs[s]
        for copy in y_copies[s]:
            copy.wait_recv()
        mine = pl.ds(pl.multiple_of(y * PIECE, PIECE), PIECE)
        sent, sent2 = 0, 0
        for t, slot in enumerate(STAGES[s]):
            value = tile[core, t, mine, :].astype(F32) + incoming[t, mine, :].astype(F32)
            for d in range(NY - 1):
                value = value + arrived[d, t].astype(F32)
            flag = None
            for term in slot:
                kind, a, n = term
                one = flag_of(*term)
                if kind in ONE_BACK:
                    flag = one if flag is None else flag + one
                elif kind == "relay":
                    ship2[n] = (value * one).astype(BF16)
                    sent2 += 1
                else:
                    target = {"own": 0, "alpha": NB, "ahead": 2 * NB}[kind] + n
                    out_ref[:, target - a - 1, a, :] = value * one
            if flag is not None:
                ship_refs[s][0][sent] = (value * flag).astype(BF16)
                sent += 1
        if sent2:
            ship2_copies[s] = send(ship2, got2, ship_send.at[NSTAGE], ship_recv.at[NSTAGE], {"dp": before2})
        if sent:
            ship_copies[s] = send(*ship_refs[s], ship_send.at[s], ship_recv.at[s], {"dp": before})

    def collect(s):
        if s in ship_copies:
            ship_copies[s].wait_recv()
        if s in ship2_copies:
            ship2_copies[s].wait_recv()
        got = 0
        for slot in STAGES[s]:
            for kind, a, n in ship_terms(slot):
                value = ship_refs[s][1][got].astype(F32)
                target = (NB if kind == "beta" else 2 * NB) + n
                if kind == "far":
                    value = value * live(live0, a, target)
                if kind == "beta" or n == 0:
                    value = value + out_ref[:, target - a - 1, a, :]
                elif a == 3:
                    value = value + got2[n].astype(F32)
                out_ref[:, target - a - 1, a, :] = value
            got += len(ship_terms(slot)) > 0
        if s in ship2_copies:
            out_ref[:, 2 * NB - 4, 3, :] = out_ref[:, 2 * NB - 4, 3, :] + got2[0].astype(F32)

    compute(0)
    presum(0)
    left[0].wait_recv()
    send_left(LX, from_next.at[0])
    right[0].wait_recv()
    compute(1)
    presum(1)
    right[3].wait_recv()
    reach = live(live1, 3, 8, KH)
    for cc in range(2):
        right_mix[1, cc] = either(reach, from_prev[3, cc], scaled[cc, 3, :, a_rows])
    send_right(RX, right_mix.at[1, 1 - core], from_prev.at[RX, 1 - core])
    send_right(RX + 1, right_mix.at[1, core], from_prev.at[RX, core])
    left[3].wait_recv()
    compute(2)
    presum(2)
    final(0)
    left[1].wait_recv()
    right[1].wait_recv()
    compute(3)
    presum(3)
    final(1)
    left[2].wait_recv()
    right[2].wait_recv()
    compute(4)
    presum(4)
    mixed_early()
    final(2)
    right[RX].wait_recv()
    mixed(1 - core)
    to_core(MIXED)
    final(3)
    right[RX + 1].wait_recv()
    mixed(core)
    presum(5)
    left[LX].wait_recv()
    compute(6)
    presum(6)
    final(4)
    collect(1)
    collect(2)
    final(5)
    collect(3)
    final(6)
    collect(4)
    collect(5)
    for copy in pending:
        copy.wait_send()


def influence(gradients, preconditioner, partners):
    dma = pltpu.SemaphoreType.DMA
    scratch = [
        pltpu.VMEM((NB, ROWS, BS), F32),
        pltpu.VMEM((ROWS, HD), F32),
        pltpu.SMEM((NB, SLOTS), jnp.int32),
        pltpu.VMEM((NB, ROWS, BS), BF16),
        pltpu.VMEM((2, NB, HALF, ROWS), BF16),
        pltpu.VMEM((NB + 1, KH, BS), BF16),
        pltpu.VMEM((NB + 1, 2, HALF, KH), BF16),
        pltpu.VMEM((2, KH, BS), BF16),
        pltpu.VMEM((2, 2, HALF, KH), BF16),
        pltpu.VMEM((2, 2, HALF, BS), F32),
        pltpu.VMEM((LIVE_ROWS, LANES), F32),
        pltpu.VMEM((LIVE_ROWS, LANES), F32),
        pltpu.VMEM((LIVE_ROWS, LANES), F32),
        pltpu.VMEM((3, PIECE, BS), BF16),
        pltpu.VMEM((3, PIECE, BS), BF16),
    ]
    for tiles in STAGES:
        n = len(tiles)
        scratch += [
            pltpu.VMEM((2, n, HALF, BS), BF16),
            pltpu.VMEM((n, HALF, BS), BF16),
            pltpu.VMEM((NY, n, PIECE, BS), BF16),
            pltpu.VMEM((NY - 1, n, PIECE, BS), BF16),
        ]
    for n in SHIP1:
        if n:
            scratch += [pltpu.VMEM((n, PIECE, BS), BF16)] * 2
    scratch += [
        dma((NB + 2,)),
        dma((2,)),
        dma((2,)),
        dma((NB + 1,)),
        dma((NB + 1,)),
        dma((NB + 2,)),
        dma((NB + 2,)),
        dma((NSTAGE,)),
        dma((NSTAGE,)),
        dma((NSTAGE, NY - 1)),
        dma((NSTAGE, NY - 1)),
        dma((NSTAGE + 1,)),
        dma((NSTAGE + 1,)),
    ]
    return pl.pallas_call(
        kernel,
        out_shape=jax.ShapeDtypeStruct((PIECE, SLOTS, NB, BS), F32),
        in_specs=[pl.BlockSpec(memory_space=pltpu.HBM)] * 3,
        out_specs=pl.BlockSpec(memory_space=pltpu.VMEM),
        scratch_shapes=scratch,
        compiler_params=pltpu.CompilerParams(
            collective_id=0, has_side_effects=True, vmem_limit_bytes=48 * 1024 * 1024
        ),
    )(*[pltpu.with_memory_space_constraint(x, pltpu.HBM) for x in (gradients, preconditioner, partners)])


def per_device(gradients, preconditioner, partners):
    tiles = influence(gradients.reshape(ROWS, NB * BS), preconditioner.reshape(ROWS, HD), partners)
    return tiles.transpose(0, 2, 1, 3)


def solution(mesh):
    in_specs = (P(None, "head", None, "dp"), P(None, "head", None, None), P("dp", None))
    out_specs = P("head", "dp", None, None)
    return jax.shard_map(
        per_device, mesh=mesh, in_specs=in_specs, out_specs=out_specs, check_vma=False
    )
```

```python
import jax
import jax.numpy as jnp
from jax import lax
from jax.experimental import pallas as pl
from jax.experimental.pallas import tpu as pltpu
from jax.sharding import PartitionSpec as P

MESH = pl.DeviceIdType.MESH
BF16 = jnp.bfloat16
F32 = jnp.float32

BS = 256
NB = 4
SLOTS = 7
ROWS = 768
LAYERS = 3
LROWS = ROWS // LAYERS
HD = 64
NY = 4
HALF = BS // 2
PIECE = HALF // NY
KH = ROWS // 2
LIVE_ROWS = 32
LANES = 128

def fold(n):
    return tuple((("alpha", a, n), ("beta", n, a)) for a in range(NB))


STAGES = (
    tuple((("own", a, b),) for a, b in ((0, 1), (0, 2), (1, 2), (1, 3), (2, 3))),
    fold(0),
    fold(3),
    fold(1),
    fold(2),
    (
        (("far", 3, 1), ("relay", 3, 0)),
        (("far", 3, 2), ("relay", 3, 1), ("far", 2, 0)),
        (("relay", 3, 2), ("far", 2, 1), ("far", 1, 0)),
    ),
    ((("ahead", 1, 0),), (("ahead", 2, 0),), (("ahead", 3, 0), ("own", 0, 3))),
)
NSTAGE = len(STAGES)
ONE_BACK = ("beta", "far")


def ship_terms(slot):
    return [term for term in slot if term[0] in ONE_BACK]


SHIP1 = [sum(len(ship_terms(slot)) > 0 for slot in slots) for slots in STAGES]
RX = LX = 4
MIXED = 5


def kernel(g_hbm, p_hbm, partners_hbm, out_ref, *scratch):
    it = iter(scratch)
    take = lambda n: [next(it) for _ in range(n)]
    gbuf, pbuf, partners_smem, plain, scaled, from_next, from_prev, left_mix, right_mix, early = take(10)
    live0, live1, live2 = take(3)
    ship2, got2 = take(2)
    stage_refs = [take(4) for _ in range(NSTAGE)]
    ship_refs = [take(2) if n else None for n in SHIP1]
    (load_sem, live_send, live_recv, left_send, left_recv, right_send, right_recv) = take(7)
    (core_send, core_recv, y_send, y_recv, ship_send, ship_recv) = take(6)

    n_dp = lax.axis_size("dp")
    dp = lax.axis_index("dp")
    head = lax.axis_index("head")
    core = lax.rem(head, 2)
    y = lax.div(head, 2)
    before, before2 = [lax.rem(dp + n_dp - d, n_dp) for d in (1, 2)]
    after, after2 = [lax.rem(dp + d, n_dp) for d in (1, 2)]
    other = head + 1 - 2 * core
    peers = [lax.rem(y + d, NY) * 2 + core for d in range(1, NY)]

    barrier = pltpu.get_barrier_semaphore()
    neighbours = (before, after, before2, after2)
    for target in neighbours:
        pl.semaphore_signal(barrier, inc=1, device_id={"dp": target}, device_id_type=MESH)
    for target in [other] + peers:
        pl.semaphore_signal(barrier, inc=1, device_id={"head": target}, device_id_type=MESH)

    loads = {}
    blocks = [(j, g_hbm.at[:, pl.ds(j * BS, BS)], gbuf.at[j]) for j in (0, 2, 3, 1)]
    tables = [("partners", partners_hbm, partners_smem), ("p", p_hbm, pbuf)]
    for name, src, dst in tables + blocks:
        load = pltpu.make_async_copy(src, dst, load_sem.at[len(loads)])
        load.start()
        loads[name] = load

    pending = []

    def send(src, dst, send_sem, recv_sem, device):
        copy = pltpu.make_async_remote_copy(
            src_ref=src,
            dst_ref=dst,
            send_sem=send_sem,
            recv_sem=recv_sem,
            device_id=device,
            device_id_type=MESH,
        )
        copy.start()
        pending.append(copy)
        return copy

    def live(ref, a, target, width=BS):
        row = a * 8 + target - a - 1
        return jnp.concatenate([ref[row : row + 1, :]] * (width // LANES), axis=1)

    def load_plain(j):
        loads[j].wait()
        plain[j] = gbuf[j].astype(BF16)

    left, right = {}, {}

    def send_left(n, src):
        left[n] = send(src, from_next.at[n], left_send.at[n], left_recv.at[n], {"dp": before})

    def send_right(n, src, dst=None):
        dst = from_prev.at[n] if dst is None else dst
        right[n] = send(src, dst, right_send.at[n], right_recv.at[n], {"dp": after})

    a_rows, b_rows = pl.ds(0, KH), pl.ds(KH, KH)

    def scale(a, layers=range(LAYERS)):
        for layer in layers:
            rows = pl.ds(layer * LROWS, LROWS)
            high = plain[a, rows, :]
            low = (gbuf[a, rows, :] - high.astype(F32)).astype(BF16)
            p_high, p_low = factors[layer]
            value = (
                jnp.dot(p_high, high, preferred_element_type=F32)
                + jnp.dot(p_low, high, preferred_element_type=F32)
                + jnp.dot(p_high, low, preferred_element_type=F32)
            )
            value = value.T.astype(BF16)
            for yy in range(NY):
                for cc in range(2):
                    scaled[cc, a, pl.ds(yy * PIECE, PIECE), rows] = value[
                        (yy * 2 + cc) * PIECE : (yy * 2 + cc + 1) * PIECE
                    ]

    def either(flag, yes, no):
        return (flag * yes.astype(F32) + (1.0 - flag) * no.astype(F32)).astype(BF16)

    row_head = lax.broadcasted_iota(jnp.int32, (LROWS, LROWS), 0) // HD
    col_head = lax.broadcasted_iota(jnp.int32, (LROWS, LROWS), 1) // HD
    diagonal = (row_head == col_head).astype(F32)
    loads["p"].wait()
    factors = []
    for layer in range(LAYERS):
        wide = jnp.concatenate([pbuf[pl.ds(layer * LROWS, LROWS), :]] * (LROWS // HD), axis=1)
        wide = (wide * diagonal).T
        high = wide.astype(BF16)
        factors.append((high, (wide - high.astype(F32)).astype(BF16)))

    loads["partners"].wait()
    live0[...] = jnp.zeros((LIVE_ROWS, LANES), F32)
    for a in range(NB):
        for k in range(SLOTS):
            slot = jnp.where(partners_smem[a, k] >= 0, 1.0, 0.0).astype(F32)
            live0[a * 8 + k : a * 8 + k + 1, :] = jnp.full((1, LANES), slot, F32)

    load_plain(0)
    scale(0, (1, 2))
    load_plain(2)
    scale(2, (0, 1))
    reach = live(live0, 2, 9, KH)
    for cc in range(2):
        right_mix[0, cc] = either(reach, scaled[cc, 2, :, a_rows], scaled[cc, 0, :, b_rows])

    pl.semaphore_wait(barrier, len(neighbours) + 1 + len(peers))
    live_copies = [
        send(live0, live1, live_send.at[0], live_recv.at[0], {"dp": after}),
        send(live0, live2, live_send.at[1], live_recv.at[1], {"dp": after2}),
    ]
    send_right(0, right_mix.at[0])
    send_left(0, plain.at[0, a_rows])
    load_plain(3)
    scale(3, (1, 2))
    send_right(3, scaled.at[:, 3, :, b_rows])
    load_plain(1)
    scale(0, (0,))
    scale(2, (2,))
    scale(3, (0,))
    for copy in live_copies:
        copy.wait_recv()
    reach = live(live2, 2, 8)
    for n in (3, 2):
        left_mix[n - 2] = either(reach, plain[n - 2, b_rows, :], plain[n, a_rows, :])
    send_left(3, left_mix.at[1])
    send_left(1, plain.at[1, a_rows])
    send_left(2, left_mix.at[0])
    scale(1)
    send_right(1, scaled.at[:, 1, :, b_rows])
    send_right(2, scaled.at[:, 2, :, b_rows])

    core_copies, y_copies, ship_copies, ship2_copies = {}, {}, {}, {}

    def own_rows(a, count, columns):
        lhs = scaled[:, a : a + count, :, columns]
        return lhs.reshape(2 * count * HALF, lhs.shape[-1])

    def product(lhs, rhs):
        return jnp.dot(lhs, rhs, preferred_element_type=F32)

    def prev_rows(n):
        return from_prev[n].reshape(BS, KH)

    def flag_of(kind, a, n):
        if kind == "relay":
            return live(live2, a, 2 * NB + n)
        if kind in ONE_BACK:
            return live(live1, a, (NB if kind == "beta" else 2 * NB) + n)
        return live(live0, a, {"own": 0, "alpha": NB, "ahead": 2 * NB}[kind] + n)

    def beta(a, n):
        return product(prev_rows(a), plain[n, b_rows, :]).reshape(2, HALF, BS) * flag_of("beta", a, n)

    def far(a, n):
        value = product(prev_rows(a), from_next[2 + n])
        if n == 1:
            value = value + product(prev_rows(0), from_next[n])
        return value.reshape(2, HALF, BS) * flag_of("far", a, n)

    def mixed_early():
        early[:, 0] = far(2, 0)
        early[:, 1] = far(2, 1) + far(1, 0)

    def mixed(half):
        tile = stage_refs[MIXED][0]
        lhs = from_prev[RX, half]
        for index, (c, n) in enumerate(((1, 0), (2, 1), (None, 2))):
            value = product(lhs, plain[n, b_rows, :]) * flag_of("relay", 3, n)
            if c is not None:
                value = value + product(lhs, from_next[c]) * flag_of("far", 3, c)
            if index:
                value = value + early[half, index - 1]
            tile[half, index] = value.astype(BF16)

    def to_core(s):
        tile, incoming, _, _ = stage_refs[s]
        core_copies[s] = send(tile.at[1 - core], incoming, core_send.at[s], core_recv.at[s], {"head": other})

    def compute(s):
        tile = stage_refs[s][0]
        kind, _, n = STAGES[s][0][0]
        if kind == "own":
            index = 0
            for b, first, count in ((1, 0, 1), (2, 0, 2), (3, 1, 2)):
                value = product(own_rows(first, count, pl.ds(0, ROWS)), plain[b])
                tile[:, index : index + count] = value.reshape(2, count, HALF, BS).astype(BF16)
                index += count
        elif kind == "ahead":
            value = product(own_rows(1, NB - 1, a_rows), from_next[LX]).reshape(2, NB - 1, HALF, BS)
            tile[:, 0:2] = value[:, 0:2].astype(BF16)
            last = product(own_rows(0, 1, pl.ds(0, ROWS)), plain[3]).reshape(2, HALF, BS)
            last = last * flag_of("own", 0, 3) + value[:, 2] * flag_of("ahead", 3, 0)
            tile[:, 2] = last.astype(BF16)
        else:
            forward = product(own_rows(0, NB, a_rows), from_next[n]).reshape(2, NB, HALF, BS)
            for a in range(NB):
                tile[:, a] = (forward[:, a] * flag_of("alpha", a, n) + beta(n, a)).astype(BF16)
        to_core(s)

    def presum(s):
        tile, incoming, pieces, arrived = stage_refs[s]
        core_copies[s].wait_recv()
        total = (tile[core].astype(F32) + incoming[...].astype(F32)).astype(BF16)
        for yy in range(NY):
            pieces[yy] = total[:, yy * PIECE : (yy + 1) * PIECE, :]
        y_copies[s] = [
            send(
                pieces.at[lax.rem(y + d, NY)],
                arrived.at[d - 1],
                y_send.at[s, d - 1],
                y_recv.at[s, d - 1],
                {"head": peers[d - 1]},
            )
            for d in range(1, NY)
        ]

    def final(s):
        tile, incoming, _, arrived = stage_refs[s]
        for copy in y_copies[s]:
            copy.wait_recv()
        mine = pl.ds(pl.multiple_of(y * PIECE, PIECE), PIECE)
        sent, sent2 = 0, 0
        for t, slot in enumerate(STAGES[s]):
            value = tile[core, t, mine, :].astype(F32) + incoming[t, mine, :].astype(F32)
            for d in range(NY - 1):
                value = value + arrived[d, t].astype(F32)
            flag = None
            for term in slot:
                kind, a, n = term
                one = flag_of(*term)
                if kind in ONE_BACK:
                    flag = one if flag is None else flag + one
                elif kind == "relay":
                    ship2[n] = (value * one).astype(BF16)
                    sent2 += 1
                else:
                    target = {"own": 0, "alpha": NB, "ahead": 2 * NB}[kind] + n
                    out_ref[:, target - a - 1, a, :] = value * one
            if flag is not None:
                ship_refs[s][0][sent] = (value * flag).astype(BF16)
                sent += 1
        if sent2:
            ship2_copies[s] = send(ship2, got2, ship_send.at[NSTAGE], ship_recv.at[NSTAGE], {"dp": before2})
        if sent:
            ship_copies[s] = send(*ship_refs[s], ship_send.at[s], ship_recv.at[s], {"dp": before})

    def collect(s):
        if s in ship_copies:
            ship_copies[s].wait_recv()
        if s in ship2_copies:
            ship2_copies[s].wait_recv()
        got = 0
        for slot in STAGES[s]:
            for kind, a, n in ship_terms(slot):
                value = ship_refs[s][1][got].astype(F32)
                target = (NB if kind == "beta" else 2 * NB) + n
                if kind == "far":
                    value = value * live(live0, a, target)
                if kind == "beta" or n == 0:
                    value = value + out_ref[:, target - a - 1, a, :]
                elif a == 3:
                    value = value + got2[n].astype(F32)
                out_ref[:, target - a - 1, a, :] = value
            got += len(ship_terms(slot)) > 0
        if s in ship2_copies:
            out_ref[:, 2 * NB - 4, 3, :] = out_ref[:, 2 * NB - 4, 3, :] + got2[0].astype(F32)

    compute(0)
    presum(0)
    left[0].wait_recv()
    send_left(LX, from_next.at[0])
    right[0].wait_recv()
    compute(1)
    presum(1)
    right[3].wait_recv()
    reach = live(live1, 3, 8, KH)
    for cc in range(2):
        right_mix[1, cc] = either(reach, from_prev[3, cc], scaled[cc, 3, :, a_rows])
    send_right(RX, right_mix.at[1, 1 - core], from_prev.at[RX, 1 - core])
    send_right(RX + 1, right_mix.at[1, core], from_prev.at[RX, core])
    left[3].wait_recv()
    compute(2)
    presum(2)
    final(0)
    left[1].wait_recv()
    right[1].wait_recv()
    compute(3)
    presum(3)
    final(1)
    left[2].wait_recv()
    right[2].wait_recv()
    compute(4)
    pl.when(core == 1)(mixed_early)
    presum(4)
    pl.when(core == 0)(mixed_early)
    final(2)
    right[RX].wait_recv()
    mixed(1 - core)
    to_core(MIXED)
    final(3)
    right[RX + 1].wait_recv()
    mixed(core)
    presum(5)
    left[LX].wait_recv()
    compute(6)
    presum(6)
    final(4)
    collect(1)
    collect(2)
    final(5)
    collect(3)
    final(6)
    collect(4)
    collect(5)
    for copy in pending:
        copy.wait_send()


def influence(gradients, preconditioner, partners):
    dma = pltpu.SemaphoreType.DMA
    scratch = [
        pltpu.VMEM((NB, ROWS, BS), F32),
        pltpu.VMEM((ROWS, HD), F32),
        pltpu.SMEM((NB, SLOTS), jnp.int32),
        pltpu.VMEM((NB, ROWS, BS), BF16),
        pltpu.VMEM((2, NB, HALF, ROWS), BF16),
        pltpu.VMEM((NB + 1, KH, BS), BF16),
        pltpu.VMEM((NB + 1, 2, HALF, KH), BF16),
        pltpu.VMEM((2, KH, BS), BF16),
        pltpu.VMEM((2, 2, HALF, KH), BF16),
        pltpu.VMEM((2, 2, HALF, BS), F32),
        pltpu.VMEM((LIVE_ROWS, LANES), F32),
        pltpu.VMEM((LIVE_ROWS, LANES), F32),
        pltpu.VMEM((LIVE_ROWS, LANES), F32),
        pltpu.VMEM((3, PIECE, BS), BF16),
        pltpu.VMEM((3, PIECE, BS), BF16),
    ]
    for tiles in STAGES:
        n = len(tiles)
        scratch += [
            pltpu.VMEM((2, n, HALF, BS), BF16),
            pltpu.VMEM((n, HALF, BS), BF16),
            pltpu.VMEM((NY, n, PIECE, BS), BF16),
            pltpu.VMEM((NY - 1, n, PIECE, BS), BF16),
        ]
    for n in SHIP1:
        if n:
            scratch += [pltpu.VMEM((n, PIECE, BS), BF16)] * 2
    scratch += [
        dma((NB + 2,)),
        dma((2,)),
        dma((2,)),
        dma((NB + 1,)),
        dma((NB + 1,)),
        dma((NB + 2,)),
        dma((NB + 2,)),
        dma((NSTAGE,)),
        dma((NSTAGE,)),
        dma((NSTAGE, NY - 1)),
        dma((NSTAGE, NY - 1)),
        dma((NSTAGE + 1,)),
        dma((NSTAGE + 1,)),
    ]
    return pl.pallas_call(
        kernel,
        out_shape=jax.ShapeDtypeStruct((PIECE, SLOTS, NB, BS), F32),
        in_specs=[pl.BlockSpec(memory_space=pltpu.HBM)] * 3,
        out_specs=pl.BlockSpec(memory_space=pltpu.VMEM),
        scratch_shapes=scratch,
        compiler_params=pltpu.CompilerParams(
            collective_id=0, has_side_effects=True, vmem_limit_bytes=48 * 1024 * 1024
        ),
    )(*[pltpu.with_memory_space_constraint(x, pltpu.HBM) for x in (gradients, preconditioner, partners)])


def per_device(gradients, preconditioner, partners):
    tiles = influence(gradients.reshape(ROWS, NB * BS), preconditioner.reshape(ROWS, HD), partners)
    return tiles.transpose(0, 2, 1, 3)


def solution(mesh):
    in_specs = (P(None, "head", None, "dp"), P(None, "head", None, None), P("dp", None))
    out_specs = P("head", "dp", None, None)
    return jax.shard_map(
        per_device, mesh=mesh, in_specs=in_specs, out_specs=out_specs, check_vma=False
    )
```
